128 devices in a mesh: dom: 128 (over y, z, x, core).
Axes of the slice: x: 4, y: 4, z: 4, core: 2. Of those that a mesh axis runs over, the one named last changes fastest.
Arguments:
- concentration: float32 [4096, 128], P('dom'), may hold values from 0 to 1
- reaction_rate: float32 [4096, 128], P('dom'), may hold values from 0.5 to 4
- step_size: float32 [1], replicated, may hold values from 1 to 2
- block_values: float32 [4096, 5, 128, 128], P('dom'), may hold values from -40 to 48, as said below
- block_columns: int32 [4096, 5], P('dom'), may hold values from 0 to 95, as said below
- row_lengths: int32 [4096], P('dom'), may hold values from 2 to 5, as said below
- send_lists: int32 [128, 4, 16], P('dom'), may hold values from 0 to 31, as said below
Outputs:
- next_concentration: float32 [4096, 128], P('dom')
The draws below stay inside these ranges and needn't reach their ends.
Inputs may be any that keep to these rules, and one draw needn't show every extreme that they name: `send_lists`: for every partition and offset index q (offsets -2, -1, +1, +2), 16 distinct local block indices. `block_columns`: slot 0 of a block row is the row's own local block; live slots name a local block (below 32) or a ghost slot 32 + q * 16 + g of a block that the partition at offset index q sends; slot 1 of local block row q, for q = 0..3, is a ghost slot of offset index q; slots at or past the row's length repeat the row's own local block. `row_lengths`: some block row has all 5 slots live. `block_values`: slot 0 of every block row holds 8 times the identity plus a full random block; the other slots hold full random blocks.
All inputs are finite; a program needn't handle non-finite values.
Results may differ from the reference program's by a relative error of at most 0.00016.
Values sent between devices are 32-bit elements; how exact they have to be, the bound alone decides.
No kernel may reach another device: no remote copies, remote signals or barrier semaphores. Data moves between devices by JAX's collectives and lax.ppermute only.
A program may use at most 64 MiB of HBM per device.

```python
import math
import jax
import jax.numpy as jnp
from jax import lax

BLK = 128
BDEV = 32
NNZB = 5
GMAX = 16
KRYLOV = 3
RESTARTS = 2
NDEV = 128
NB = 4096


def ghost_counts(key):
    first_key, second_key = jax.random.split(jax.random.fold_in(key, 11))
    counts = jax.random.randint(first_key, (NDEV, 4), max(GMAX // 4, 1), GMAX + 1)
    fullest = jax.random.randint(second_key, (4,), 0, NDEV)
    devices = jnp.arange(NDEV)[:, None]
    return jnp.where(devices == fullest[None, :], GMAX, counts).astype(jnp.int32)


def lengths_drawn(key):
    first_key, second_key = jax.random.split(jax.random.fold_in(key, 23))
    lengths = jax.random.randint(first_key, (NB,), 2, NNZB + 1)
    longest = jax.random.randint(second_key, (), 0, NB)
    return jnp.where(jnp.arange(NB) == longest, NNZB, lengths).astype(jnp.int32)


def draw_row_lengths(key, part):
    return lengths_drawn(key)


def draw_send_lists(key, part):
    scores = jax.random.randint(jax.random.fold_in(key, 37), (NDEV, 4, BDEV), 0, 1 << 20) * BDEV + jnp.arange(BDEV)
    ordering = jnp.argsort(scores, axis=-1)
    return ordering[:, :, :GMAX].astype(jnp.int32)


def draw_block_columns(key, part):
    counts = ghost_counts(key)
    lengths = lengths_drawn(key)
    subkeys = jax.random.split(jax.random.fold_in(key, 53), 4)
    row_ids = jnp.arange(NB)
    device = row_ids // BDEV
    local_row = row_ids % BDEV
    positions = jnp.arange(NNZB)[None, :]
    forced = (positions == 1) & (local_row[:, None] < 4)
    variety = jax.random.randint(subkeys[0], (NB, NNZB), 0, 2)
    variety = jnp.where(forced, 1, variety)
    owned = jax.random.randint(subkeys[1], (NB, NNZB), 0, BDEV)
    within = jax.random.randint(subkeys[2], (NB, NNZB), 0, 4)
    within = jnp.where(forced, jnp.broadcast_to((local_row % 4)[:, None], (NB, NNZB)), within)
    drawn_bits = jax.random.randint(subkeys[3], (NB, NNZB), 0, 1 << 20)
    offsets = jnp.array([-2, -1, 1, 2])
    sender = (device[:, None] - offsets[within]) % NDEV
    ghost_slot = drawn_bits % counts[sender, within]
    ghost = BDEV + within * GMAX + ghost_slot
    picked = jnp.where(variety == 1, ghost, owned)
    picked = jnp.where(positions == 0, local_row[:, None], picked)
    picked = jnp.where(positions < lengths[:, None], picked, local_row[:, None])
    return picked.astype(jnp.int32)


def draw_block_values(key, part):
    first_key = jax.random.fold_in(jax.random.fold_in(key, 71), 0)
    spread = 4.0 / math.sqrt(BLK * NNZB)
    shape = (NB, NNZB, BLK, BLK)
    entries = jax.random.normal(first_key, shape, jnp.float32)
    diagonal = (jnp.arange(NNZB) == 0).astype(jnp.float32)[None, :, None, None] * jnp.eye(BLK, dtype=jnp.float32)[None, None] * 8.0
    return (entries * spread + diagonal).astype(jnp.float32)


def block_scale(own_key, extent, shards, low, high):
    loudness = 1.0
    for dim, blocks in shards:
        draws = jax.random.uniform(jax.random.fold_in(jax.random.fold_in(own_key, 6), dim), (blocks,), jnp.float32, low / len(shards), high / len(shards))
        loudness = loudness * jnp.repeat(jnp.exp(draws), extent[dim] // blocks).reshape((-1,) + (1,) * (len(extent) - 1 - dim))
    return loudness


def setup_inputs(seed: int = 0) -> dict:
    key_of = jax.random.split(jax.random.key(seed), 8)
    return {
        "concentration": jnp.clip(1.0 * jax.random.uniform(key_of[0], (NB, BLK), jnp.float32) ** block_scale(key_of[0], (NB, BLK), ((0, 128),), -0.2, 0.2), 0.0, 1.0),
        "reaction_rate": jnp.clip(jnp.exp(math.log(4.0) - 2.0794415 * jax.random.uniform(key_of[1], (NB, BLK), jnp.float32) ** block_scale(key_of[1], (NB, BLK), ((0, 128),), -0.2, 0.2)), 0.5, 4.0),
        "step_size": jnp.clip(jax.random.uniform(key_of[2], (1,), jnp.float32, 1.0, 2.0), 1.0, 2.0),
        "block_values": draw_block_values(jax.random.fold_in(key_of[7], 71), 0),
        "block_columns": draw_block_columns(jax.random.fold_in(key_of[7], 71), 0),
        "row_lengths": draw_row_lengths(jax.random.fold_in(key_of[7], 71), 0),
        "send_lists": draw_send_lists(jax.random.fold_in(key_of[7], 71), 0),
    }


epsilon = 1e-06
OFFSETS = (-2, -1, 1, 2)

def column_map(block_columns, send_lists):
    device = (jnp.arange(NB, dtype=jnp.int32) // BDEV)[:, None]
    ghost_index = jnp.maximum(block_columns - BDEV, 0)
    neighbour = ghost_index // GMAX
    ghost_slot = ghost_index % GMAX
    offsets = jnp.array(OFFSETS, jnp.int32)
    sender = (device - offsets[neighbour]) % NDEV
    remote = send_lists[sender, neighbour, ghost_slot]
    owned = device * BDEV + block_columns
    return jnp.where(block_columns < BDEV, owned, sender * BDEV + remote).astype(jnp.int32)

def product(block_values, columns, active, field):
    gathered = field[columns] * active[:, :, None]
    return jnp.einsum('bsij,bsj->bi', block_values, gathered, precision=lax.Precision.HIGHEST)

def phi_column(hessenberg, substep):
    order = hessenberg.shape[0]
    augmented = jnp.zeros((order + 1, order + 1), jnp.float32)
    augmented = augmented.at[:order, :order].set(substep * hessenberg).at[0, order].set(1.0)
    reduced = augmented / 64.0
    identity = jnp.eye(order + 1, dtype=jnp.float32)
    series = identity
    for degree in range(12, 0, -1):
        series = identity + jnp.dot(reduced, series, precision=lax.Precision.HIGHEST) / degree
    for square_turn in range(6):
        series = jnp.dot(series, series, precision=lax.Precision.HIGHEST)
    return series[:order, order]

def krylov(start, apply):
    magnitude = jnp.sqrt(jnp.sum(start * start) + epsilon)
    vectors = jnp.zeros((KRYLOV,) + start.shape, jnp.float32).at[0].set(start / magnitude)
    hessenberg = jnp.zeros((KRYLOV, KRYLOV), jnp.float32)
    for column in range(KRYLOV):
        mapped = apply(vectors[column])
        projection = jnp.einsum('kbi,bi->k', vectors, mapped, precision=lax.Precision.HIGHEST)
        mapped = mapped - jnp.einsum('k,kbi->bi', projection, vectors, precision=lax.Precision.HIGHEST)
        hessenberg = hessenberg.at[:, column].set(projection)
        if column + 1 < KRYLOV:
            length = jnp.sqrt(jnp.sum(mapped * mapped) + epsilon)
            hessenberg = hessenberg.at[column + 1, column].set(length)
            vectors = vectors.at[column + 1].set(mapped / length)
    return (magnitude, vectors, hessenberg)

def reference(concentration, reaction_rate, step_size, block_values, block_columns, row_lengths, send_lists):
    columns = column_map(block_columns, send_lists)
    active = (jnp.arange(NNZB, dtype=jnp.int32)[None, :] < row_lengths[:, None]).astype(jnp.float32)
    slope = reaction_rate * (1.0 - 2.0 * concentration)

    def apply(field):
        return slope * field - product(block_values, columns, active, field)
    forcing = reaction_rate * concentration * (1.0 - concentration) - product(block_values, columns, active, concentration)
    substep = step_size[0] / RESTARTS
    increment = jnp.zeros_like(concentration)
    for restart in range(RESTARTS):
        start = forcing if restart == 0 else apply(increment) + forcing
        magnitude, vectors, hessenberg = krylov(start, apply)
        weights = phi_column(hessenberg, substep)
        increment = increment + substep * magnitude * jnp.einsum('k,kbi->bi', weights, vectors, precision=lax.Precision.HIGHEST)
    return concentration + increment
```

```python
import jax
import jax.numpy as jnp
from jax import lax
from jax.experimental import pallas as pl
from jax.experimental.pallas import tpu as pltpu
from jax.sharding import PartitionSpec as P

BLK = 128
ROWS = 32
SLOTS = 5
GHOST = 16
ENTRIES = ROWS * SLOTS
DEGREE = 6
SHIFT = 8.0
SCALE = 0.25
PAIRS = [(a, b) for b in range(DEGREE + 1) for a in range(min(b, DEGREE - 1) + 1)]

FIRST = 0
LAST = 32
REMOTE = 64
COLUMN = 128
SEND = 288
TABLE = 384

f32 = jnp.float32
bf16 = jnp.bfloat16


def vmem(n=1):
    return [pl.BlockSpec(memory_space=pltpu.VMEM)] * n


def smem(n=1):
    return [pl.BlockSpec(memory_space=pltpu.SMEM)] * n


def exchanges(devices):
    two = [(p, (p + 2) % devices) for p in range(devices)]
    one = [(p, (p + 1) % devices) for p in range(devices)]
    picked = (
        [e for e in two if e[0] % 4 >= 2],
        [e for e in one if e[0] % 2 == 1],
        [e for e in two if e[0] % 4 < 2],
        [e for e in one if e[0] % 2 == 0],
    )
    return [[(a, b) for a, b in es] + [(b, a) for a, b in es] for es in picked]


def roles():
    place = lax.axis_index("dom")
    even = (place % 2) == 0
    low = (place % 4) < 2
    pick = lambda c, a, b: jnp.where(c, jnp.int32(a), jnp.int32(b))
    return pick(low, 0, 3), pick(even, 1, 2), pick(low, 3, 0), pick(even, 2, 1)


def write_packets(field, row_of, packets):
    for t in range(4):
        for g in range(GHOST):
            packets[t][g : g + 1, :] = field[pl.ds(row_of(t, g), 1), :]


def first_packets(send, field, *packets):
    by = roles()
    write_packets(field, lambda t, g: send[0, by[t], g], packets)


def partial_products(table, begin, end, place, blocks, field, pieces):
    def row(b, carry):
        def entry(e, total):
            at = place(e)
            return total + blocks[at] * field[pl.ds(table[COLUMN + at], 1), :]

        total = lax.fori_loop(begin(b), end(b), entry, jnp.zeros((BLK, BLK), f32))
        span = pl.ds(pl.multiple_of(b * BLK, BLK), BLK)
        high = total.astype(bf16)
        rest = total - high.astype(f32)
        middle = rest.astype(bf16)
        pieces[0, span, :] = high
        pieces[1, span, :] = middle
        pieces[2, span, :] = (rest - middle.astype(f32)).astype(bf16)
        return carry

    lax.fori_loop(0, ROWS, row, 0)


def column_sums(pieces, out):
    ones = jnp.ones((8, BLK), bf16)
    for b in range(ROWS):
        total = sum(
            lax.dot_general(
                ones,
                pieces[k, b * BLK : (b + 1) * BLK, :],
                (((1,), (1,)), ((), ())),
                preferred_element_type=f32,
            )
            for k in range(3)
        )
        out[b : b + 1, :] = total[0:1]


def local_product(table, blocks, field, pieces, out):
    partial_products(
        table,
        lambda b: table[FIRST + b],
        lambda b: table[LAST + b],
        lambda e: e,
        blocks,
        field,
        pieces,
    )
    column_sums(pieces, out)


def setup(columns, lengths, send, values, field, rate, blocks, table, out, pieces, done):
    by = roles()
    place = lax.axis_index("dom")
    even = (place % 2) == 0
    low = (place % 4) < 2
    at = (
        jnp.where(low, 2, 0),
        jnp.where(even, 3, 1),
        jnp.where(even, 1, 3),
        jnp.where(low, 0, 2),
    )

    def row(b, carry):
        near, far = carry
        length = lengths[b]
        table[FIRST + b] = near
        table[REMOTE + b] = far
        last = near
        for s in range(SLOTS):
            column = columns[b, s]
            live = s < length
            ghost = jnp.logical_and(live, column >= ROWS)
            index = jnp.maximum(column - ROWS, 0)
            q = index // GHOST
            spot = jnp.where(q < 2, jnp.where(q == 0, at[0], at[1]), jnp.where(q == 2, at[2], at[3]))
            target = jnp.where(ghost, ENTRIES - 1 - far, near)
            table[COLUMN + target] = jnp.where(ghost, spot * GHOST + index % GHOST, column)
            pltpu.make_async_copy(values.at[b, s], blocks.at[target], done).start()
            one = ghost.astype(jnp.int32)
            far = far + one
            near = near + 1 - one
            last = jnp.where(live, near, last)
        table[LAST + b] = last
        return near, far

    _, far = lax.fori_loop(0, ROWS, row, (jnp.int32(0), jnp.int32(0)))
    table[REMOTE + ROWS] = far
    for t in range(4):
        for g in range(GHOST):
            table[SEND + t * GHOST + g] = send[0, by[t], g]
    pltpu.make_async_copy(blocks, blocks, done).wait()
    local_product(table, blocks, field, pieces, out)
    out[...] = rate[...] * field[...] * (1.0 - field[...]) - out[...]


def near_part(table, blocks, field, rate, concentration, out, pieces):
    local_product(table, blocks, field, pieces, out)
    slope = rate[...] * (1.0 - 2.0 * concentration[...]) + SHIFT
    out[...] = slope * field[...] - out[...]


def ghost_product(table, blocks, near, arrived, out, ghosts, pieces, scale):
    for t in range(4):
        ghosts[t * GHOST : (t + 1) * GHOST, :] = arrived[t][...]
    partial_products(
        table,
        lambda b: table[REMOTE + b],
        lambda b: table[REMOTE + b + 1],
        lambda e: ENTRIES - 1 - e,
        blocks,
        ghosts,
        pieces,
    )
    column_sums(pieces, out)
    out[...] = (near[...] - out[...]) * scale


def far_part(scale):
    def kernel(table, blocks, near, g0, g1, g2, g3, out, p0, p1, p2, p3, ghosts, pieces):
        ghost_product(table, blocks, near, (g0, g1, g2, g3), out, ghosts, pieces, scale)
        write_packets(out, lambda t, g: table[SEND + t * GHOST + g], (p0, p1, p2, p3))

    return kernel


def last_part(table, blocks, near, g0, g1, g2, g3, *rest):
    basis = rest[:DEGREE]
    sums, out, ghosts, pieces, rows = rest[DEGREE:]
    ghost_product(table, blocks, near, (g0, g1, g2, g3), out, ghosts, pieces, SCALE)
    basis = basis + (out,)
    rows[...] = jnp.zeros((BLK, BLK), f32)
    for k, (a, b) in enumerate(PAIRS):
        both = basis[a][...] * basis[b][...]
        rows[k : k + 1, :] = jnp.sum(both, axis=0, keepdims=True)
    line = lax.dot_general(
        jnp.ones((8, BLK), f32),
        rows[...],
        (((1,), (1,)), ((), ())),
        precision=lax.Precision.HIGHEST,
        preferred_element_type=f32,
    )
    sums[...] = jnp.broadcast_to(line[0:1], sums.shape)


def add(x, y):
    if x is None:
        return y
    return x if y is None else x + y


def times(x, y):
    return None if x is None or y is None else x * y


def minus(x, y):
    if y is None:
        return x
    return -y if x is None else x - y


def jacobian(v):
    out = [None if x is None else x * -SHIFT for x in v]
    for k in range(DEGREE):
        if v[k] is not None:
            out[k + 1] = add(out[k + 1], v[k] * (1.0 / SCALE))
    return out


def through(gram, v):
    return [
        (lambda terms: None if not terms else sum(terms[1:], terms[0]))(
            [gram[min(a, b), max(a, b)] * v[b] for b in range(DEGREE + 1) if v[b] is not None and (a, b) != (DEGREE, DEGREE)]
        )
        for a in range(DEGREE + 1)
    ]


def dot(u, v):
    terms = [x * y for x, y in zip(u, v) if x is not None and y is not None]
    return sum(terms[1:], terms[0])


def scaled(v, x):
    return [None if y is None else y * x for y in v]


def phi_weights(h, substep):
    n = len(h)
    reduced = [[None if x is None else x * substep * (1.0 / 64.0) for x in r] for r in h]
    matmul = lambda p, q: [
        [
            (lambda ts: None if not ts else sum(ts[1:], ts[0]))(
                [p[i][k] * q[k][j] for k in range(n) if p[i][k] is not None and q[k][j] is not None]
            )
            for j in range(n)
        ]
        for i in range(n)
    ]
    apply = lambda p, q: [
        (lambda ts: None if not ts else sum(ts[1:], ts[0]))(
            [p[i][k] * q[k] for k in range(n) if p[i][k] is not None and q[k] is not None]
        )
        for i in range(n)
    ]
    block = [[1.0 if i == j else None for j in range(n)] for i in range(n)]
    column = [None] * n
    for degree in range(12, 0, -1):
        inverse = 1.0 / degree
        block = matmul(reduced, block)
        block = [[None if x is None else x * inverse for x in r] for r in block]
        for i in range(n):
            block[i][i] = add(block[i][i], 1.0)
        column = apply(reduced, column)
        column[0] = add(column[0], 1.0 / 64.0)
        column = [None if x is None else x * inverse for x in column]
    for turn in range(6):
        moved = apply(block, column)
        column = [add(x, y) for x, y in zip(moved, column)]
        block = matmul(block, block)
    return column


def finish(step, everyone, concentration, *rest):
    basis, out = rest[:DEGREE], rest[DEGREE]
    total = jnp.sum(everyone[...], axis=0, keepdims=True)
    gram = {
        pair: jnp.broadcast_to(total[:, k : k + 1], (8, BLK)) for k, pair in enumerate(PAIRS)
    }
    substep = jnp.full((8, BLK), step[0] * 0.5, f32)
    one = jnp.ones((8, BLK), f32)
    forcing = [one] + [None] * DEGREE
    increment = [None] * (DEGREE + 1)
    for restart in range(2):
        start = forcing if restart == 0 else [add(x, y) for x, y in zip(jacobian(increment), forcing)]
        magnitude = jnp.sqrt(dot(start, through(gram, start)) + 1e-6)
        vectors = [scaled(start, 1.0 / magnitude)]
        hessenberg = [[None] * 3 for _ in range(3)]
        for j in range(3):
            mapped = jacobian(vectors[j])
            seen = through(gram, mapped)
            weights = [dot(v, seen) for v in vectors]
            for k, weight in enumerate(weights):
                hessenberg[k][j] = weight
            if j < 2:
                for v, weight in zip(vectors, weights):
                    mapped = [minus(x, times(y, weight)) for x, y in zip(mapped, v)]
                length = jnp.sqrt(dot(mapped, through(gram, mapped)) + 1e-6)
                hessenberg[j + 1][j] = length
                vectors.append(scaled(mapped, 1.0 / length))
        phi = phi_weights(hessenberg, substep)
        for v, weight in zip(vectors, phi):
            factor = substep * magnitude * weight
            increment = [add(x, times(y, factor)) for x, y in zip(increment, v)]
    for i in range(ROWS // 8):
        span = slice(8 * i, 8 * i + 8)
        line = concentration[span, :]
        for k in range(DEGREE):
            if increment[k] is not None:
                line = line + increment[k] * basis[k][span, :]
        out[span, :] = line


LIMIT = 16 << 20
FIELD = jax.ShapeDtypeStruct((ROWS, BLK), f32)
PACKETS = [jax.ShapeDtypeStruct((GHOST, BLK), f32)] * 4
PIECES = pltpu.VMEM((3, ROWS * BLK, BLK), bf16)
GHOSTS = pltpu.VMEM((4 * GHOST, BLK), f32)


def params():
    return pltpu.CompilerParams(vmem_limit_bytes=LIMIT)


def cost(flops):
    return pl.CostEstimate(flops=flops, bytes_accessed=0, transcendentals=0)


def shards(pairs, concentration, rate, step, values, columns, lengths, send):
    devices = BLK

    def exchange(packets):
        return [lax.ppermute(x, "dom", by) for x, by in zip(packets, pairs)]

    packets = pl.pallas_call(
        first_packets,
        out_shape=PACKETS,
        in_specs=smem() + vmem(),
        out_specs=vmem(4),
        compiler_params=params(),
        name="first_packets",
    )(send, concentration)
    arrived = exchange(packets)
    blocks, table, near = pl.pallas_call(
        setup,
        out_shape=[pltpu.VMEM((ENTRIES, BLK, BLK), f32), pltpu.SMEM((TABLE,), jnp.int32), FIELD],
        in_specs=smem(3) + [pl.BlockSpec(memory_space=pl.ANY)] + vmem(2),
        out_specs=vmem() + smem() + vmem(),
        scratch_shapes=[PIECES, pltpu.SemaphoreType.DMA(())],
        compiler_params=params(),
        cost_estimate=cost(10**10),
        name="setup",
    )(columns, lengths, send, values, concentration, rate)
    blocks = pltpu.with_memory_space_constraint(blocks, pltpu.VMEM)
    table = pltpu.with_memory_space_constraint(table, pltpu.SMEM)
    basis = []
    for k in range(DEGREE):
        field, *packets = pl.pallas_call(
            far_part(1.0 if k == 0 else SCALE),
            out_shape=[FIELD] + PACKETS,
            in_specs=smem() + vmem(6),
            out_specs=vmem(5),
            scratch_shapes=[GHOSTS, PIECES],
            compiler_params=params(),
            name="far_part",
        )(table, blocks, near, *arrived)
        basis.append(field)
        arrived = exchange(packets)
        near = pl.pallas_call(
            near_part,
            out_shape=FIELD,
            in_specs=smem() + vmem(4),
            out_specs=vmem()[0],
            scratch_shapes=[PIECES],
            compiler_params=params(),
            cost_estimate=cost(10**10),
            name="near_part",
        )(table, blocks, field, rate, concentration)
    sums = pl.pallas_call(
        last_part,
        out_shape=jax.ShapeDtypeStruct((devices, BLK), f32),
        in_specs=smem() + vmem(6 + DEGREE),
        out_specs=vmem()[0],
        scratch_shapes=[pltpu.VMEM((ROWS, BLK), f32), GHOSTS, PIECES, pltpu.VMEM((BLK, BLK), f32)],
        compiler_params=params(),
        name="last_part",
    )(table, blocks, near, *arrived, *basis)
    everyone = lax.all_to_all(sums, "dom", split_axis=0, concat_axis=0, tiled=True)
    return pl.pallas_call(
        finish,
        out_shape=FIELD,
        in_specs=smem() + vmem(2 + DEGREE),
        out_specs=vmem()[0],
        compiler_params=params(),
        name="finish",
    )(step, everyone, concentration, *basis)


def solution(mesh):
    pairs = exchanges(mesh.shape["dom"])

    def run(*arrays):
        return shards(pairs, *arrays)

    split = P("dom")
    return jax.shard_map(
        run,
        mesh=mesh,
        in_specs=(split, split, P(), split, split, split, split),
        out_specs=split,
        check_vma=False,
    )
```

```python
import jax
import jax.numpy as jnp
from jax import lax
from jax.experimental import pallas as pl
from jax.experimental.pallas import tpu as pltpu
from jax.sharding import PartitionSpec as P

BLK = 128
ROWS = 32
SLOTS = 5
GHOST = 16
ENTRIES = ROWS * SLOTS
DEGREE = 6
SHIFT = 8.0
SCALE = 0.25
PAIRS = [(a, b) for b in range(DEGREE + 1) for a in range(min(b, DEGREE - 1) + 1)]

FIRST = 0
LAST = 32
LOCAL = 64
GROUP = 32
LIST = 128 + GROUP
FAR = 224
MID = FAR + 3 * LIST
SEND = MID + 3 * LIST
COUNTS = SEND + 64
TABLE = 1280
CHUNKS = 8

f32 = jnp.float32
bf16 = jnp.bfloat16


def vmem(n=1):
    return [pl.BlockSpec(memory_space=pltpu.VMEM)] * n


def smem(n=1):
    return [pl.BlockSpec(memory_space=pltpu.SMEM)] * n


def exchanges(devices):
    two = [(p, (p + 2) % devices) for p in range(devices)]
    one = [(p, (p + 1) % devices) for p in range(devices)]
    picked = (
        [e for e in two if e[0] % 4 >= 2],
        [e for e in one if e[0] % 2 == 1],
        [e for e in two if e[0] % 4 < 2],
        [e for e in one if e[0] % 2 == 0],
    )
    return [[(a, b) for a, b in es] + [(b, a) for a, b in es] for es in picked]


def roles():
    place = lax.axis_index("dom")
    even = (place % 2) == 0
    low = (place % 4) < 2
    pick = lambda c, a, b: jnp.where(c, jnp.int32(a), jnp.int32(b))
    return pick(low, 0, 3), pick(even, 1, 2), pick(low, 3, 0), pick(even, 2, 1)


def write_packets(field, row_of, packets):
    for t in range(4):
        for g in range(GHOST):
            packets[t][g : g + 1, :] = field[pl.ds(row_of(t, g), 1), :]


def first_packets(send, concentration, rate, field, speed, table, p0, p1, p2, p3, done):
    copies = [
        pltpu.make_async_copy(send, table, done.at[0]),
        pltpu.make_async_copy(concentration, field, done.at[1]),
        pltpu.make_async_copy(rate, speed, done.at[2]),
    ]
    for copy in copies:
        copy.start()
    by = roles()
    for copy in copies:
        copy.wait()
    write_packets(field, lambda t, g: table[0, by[t], g], (p0, p1, p2, p3))


def split(x):
    high = x.astype(bf16)
    return high, (x - high.astype(f32)).astype(bf16)


def local_rows(table, blocks, field, pieces, begin, end):
    def row(b, carry):
        def entry(e, total):
            word = table[LOCAL + e]
            return total + blocks[word >> 6] * field[pl.ds(word & 63, 1), :]

        total = lax.fori_loop(table[FIRST + b], table[LAST + b], entry, jnp.zeros((BLK, BLK), f32))
        span = pl.ds(pl.multiple_of(b * BLK, BLK), BLK)
        high, low = split(total)
        pieces[span, 0:BLK] = high
        pieces[span, BLK : 2 * BLK] = low
        return carry

    lax.fori_loop(begin, end, row, 0)


def column_sums(pieces, out):
    ones = jnp.ones((8, 2 * BLK), bf16)
    for b in range(0, ROWS, 2):
        total = lax.dot_general(
            ones,
            pieces[b * BLK : (b + 2) * BLK, :],
            (((1,), (1,)), ((), ())),
            preferred_element_type=f32,
        )
        out[b : b + 1, :] = total[0:1, 0:BLK]
        out[b + 1 : b + 2, :] = total[0:1, BLK : 2 * BLK]


def setup(columns, lengths, send, values, field, rate, blocks, turned, table, out, where, length_of, pieces, done, small):
    step = ROWS // CHUNKS
    copies = [pltpu.make_async_copy(columns, where, small.at[0]), pltpu.make_async_copy(lengths, length_of, small.at[1])]
    for copy in copies:
        copy.start()
    for k in range(CHUNKS):
        part = pl.ds(k * step * SLOTS, step * SLOTS)
        pltpu.make_async_copy(values.at[part], blocks.at[part], done.at[k]).start()
    by = roles()
    place = lax.axis_index("dom")
    even = (place % 2) == 0
    low = (place % 4) < 2
    at = (
        jnp.where(low, 2, 0),
        jnp.where(even, 3, 1),
        jnp.where(even, 1, 3),
        jnp.where(low, 0, 2),
    )
    for t in range(4):
        for g in range(GHOST):
            table[SEND + t * GHOST + g] = send[0, by[t], g]
    for copy in copies:
        copy.wait()

    def row(b, carry):
        near, far, mid = carry
        length = length_of[b]
        table[FIRST + b] = near
        for s in range(SLOTS):
            column = where[s, b]
            live = s < length
            ghost = jnp.logical_and(live, column >= ROWS)
            index = jnp.maximum(column - ROWS, 0)
            q = index // GHOST
            spot = jnp.where(q < 2, jnp.where(q == 0, at[0], at[1]), jnp.where(q == 2, at[2], at[3]))
            first = jnp.logical_and(ghost, spot < 2)
            second = jnp.logical_and(ghost, spot >= 2)
            home = jnp.logical_and(live, column < ROWS)
            slot = b * SLOTS + s

            @pl.when(home)
            def _(near=near):
                table[LOCAL + near] = slot * 64 + column

            @pl.when(ghost)
            def _(far=far, mid=mid):
                base = jnp.where(first, FAR + far, MID + mid)
                table[base] = (spot % 2) * GHOST + index % GHOST
                table[base + LIST] = slot
                table[base + 2 * LIST] = b

            near = near + home.astype(jnp.int32)
            far = far + first.astype(jnp.int32)
            mid = mid + second.astype(jnp.int32)
        table[LAST + b] = near
        return near, far, mid

    zero = jnp.int32(0)
    _, far, mid = lax.fori_loop(0, ROWS, row, (zero, zero, zero))
    table[COUNTS] = far
    table[COUNTS + 1] = mid
    for base, count in ((FAR, far), (MID, mid)):

        def fill(i, carry, base=base, count=count):
            table[base + count + i] = 2 * GHOST
            table[base + LIST + count + i] = table[base + LIST]
            table[base + 2 * LIST + count + i] = 0
            return carry

        lax.fori_loop(0, GROUP, fill, 0)
    for k in range(CHUNKS):
        part = pl.ds(k * step * SLOTS, step * SLOTS)
        pltpu.make_async_copy(values.at[part], blocks.at[part], done.at[k]).wait()
        local_rows(table, blocks, field, pieces, k * step, (k + 1) * step)
    column_sums(pieces, out)
    out[...] = rate[...] * field[...] * (1.0 - field[...]) - out[...]
    for base, count, start, sign in ((FAR, far, 0, 1), (MID, mid, 127, -1)):

        def turn(c, carry, base=base, count=count, start=start, sign=sign):
            for u in range(4):
                i = c * 4 + u
                slot = table[base + LIST + i]
                to = jnp.where(i < count, i, 0)
                high, rest = split(jnp.transpose(blocks[slot]))
                turned[start + sign * to, :, 0:BLK] = high
                turned[start + sign * to, :, BLK : 2 * BLK] = rest
            return carry

        lax.fori_loop(0, (count + 3) // 4, turn, 0)

        def rename(i, carry, base=base, count=count, start=start, sign=sign):
            table[base + LIST + i] = start + sign * jnp.where(i < count, i, 0)
            return carry

        lax.fori_loop(0, count + GROUP, rename, 0)


def near_part(table, blocks, field, rate, concentration, out, pieces):
    local_rows(table, blocks, field, pieces, 0, ROWS)
    column_sums(pieces, out)
    slope = rate[...] * (1.0 - 2.0 * concentration[...]) + SHIFT
    out[...] = slope * field[...] - out[...]


def ghost_product(table, base, count, turned, arrived, ghosts, stage, sums):
    ghosts[0:GHOST, :] = arrived[0][...]
    ghosts[GHOST : 2 * GHOST, :] = arrived[1][...]
    ghosts[2 * GHOST : 2 * GHOST + 8, :] = jnp.zeros((8, BLK), f32)
    for ref in sums:
        ref[...] = jnp.zeros((ROWS, BLK), f32)

    def group(c, carry):
        first = base + c * GROUP
        for u in range(GROUP):
            stage[u : u + 1, :] = ghosts[pl.ds(table[first + u], 1), :]
        for v in range(0, GROUP, 8):
            left = jnp.concatenate(split(stage[v : v + 8, :]), axis=0)
            for u in range(v, v + 8):
                got = jnp.dot(left, turned[table[first + LIST + u]], preferred_element_type=f32)
                both = got[:, 0:BLK] + got[:, BLK : 2 * BLK]
                line = both[0:8] + both[8:16]
                to = pl.ds(table[first + 2 * LIST + u], 1)
                ref = sums[u % 4]
                ref[to, :] = ref[to, :] + line[u - v : u - v + 1, :]
        return carry

    lax.fori_loop(0, (count + GROUP - 1) // GROUP, group, 0)
    return (sums[0][...] + sums[1][...]) + (sums[2][...] + sums[3][...])


def middle_part(table, turned, near, g2, g3, out, ghosts, stage, *sums):
    total = ghost_product(table, MID, table[COUNTS + 1], turned, (g2, g3), ghosts, stage, sums)
    out[...] = near[...] - total


def far_part(scale):
    def kernel(table, turned, near, g0, g1, out, p0, p1, p2, p3, ghosts, stage, *sums):
        total = ghost_product(table, FAR, table[COUNTS], turned, (g0, g1), ghosts, stage, sums)
        out[...] = (near[...] - total) * scale
        write_packets(out, lambda t, g: table[SEND + t * GHOST + g], (p0, p1, p2, p3))

    return kernel


def last_part(table, turned, near, g0, g1, *rest):
    basis = rest[:DEGREE]
    sums, out, rows, ghosts, stage, *partial = rest[DEGREE:]
    total = ghost_product(table, FAR, table[COUNTS], turned, (g0, g1), ghosts, stage, partial)
    out[...] = (near[...] - total) * SCALE
    basis = basis + (out,)
    rows[...] = jnp.zeros((BLK, BLK), f32)
    for k, (a, b) in enumerate(PAIRS):
        both = basis[a][...] * basis[b][...]
        rows[k : k + 1, :] = jnp.sum(both, axis=0, keepdims=True)
    line = lax.dot_general(
        jnp.ones((8, BLK), f32),
        rows[...],
        (((1,), (1,)), ((), ())),
        precision=lax.Precision.HIGHEST,
        preferred_element_type=f32,
    )
    sums[...] = jnp.broadcast_to(line[0:1], sums.shape)


def add(x, y):
    if x is None:
        return y
    return x if y is None else x + y


def times(x, y):
    return None if x is None or y is None else x * y


def minus(x, y):
    if y is None:
        return x
    return -y if x is None else x - y


def jacobian(v):
    out = [None if x is None else x * -SHIFT for x in v]
    for k in range(DEGREE):
        if v[k] is not None:
            out[k + 1] = add(out[k + 1], v[k] * (1.0 / SCALE))
    return out


def through(gram, v):
    return [
        (lambda terms: None if not terms else sum(terms[1:], terms[0]))(
            [gram[min(a, b), max(a, b)] * v[b] for b in range(DEGREE + 1) if v[b] is not None and (a, b) != (DEGREE, DEGREE)]
        )
        for a in range(DEGREE + 1)
    ]


def dot(u, v):
    terms = [x * y for x, y in zip(u, v) if x is not None and y is not None]
    return sum(terms[1:], terms[0])


def scaled(v, x):
    return [None if y is None else y * x for y in v]


def phi_weights(h, substep):
    n = len(h)
    reduced = [[None if x is None else x * substep * (1.0 / 64.0) for x in r] for r in h]
    matmul = lambda p, q: [
        [
            (lambda ts: None if not ts else sum(ts[1:], ts[0]))(
                [p[i][k] * q[k][j] for k in range(n) if p[i][k] is not None and q[k][j] is not None]
            )
            for j in range(n)
        ]
        for i in range(n)
    ]
    apply = lambda p, q: [
        (lambda ts: None if not ts else sum(ts[1:], ts[0]))(
            [p[i][k] * q[k] for k in range(n) if p[i][k] is not None and q[k] is not None]
        )
        for i in range(n)
    ]
    block = [[1.0 if i == j else None for j in range(n)] for i in range(n)]
    column = [None] * n
    for degree in range(12, 0, -1):
        inverse = 1.0 / degree
        block = matmul(reduced, block)
        block = [[None if x is None else x * inverse for x in r] for r in block]
        for i in range(n):
            block[i][i] = add(block[i][i], 1.0)
        column = apply(reduced, column)
        column[0] = add(column[0], 1.0 / 64.0)
        column = [None if x is None else x * inverse for x in column]
    for _ in range(6):
        moved = apply(block, column)
        column = [add(x, y) for x, y in zip(moved, column)]
        block = matmul(block, block)
    return column


def finish(step, everyone, concentration, *rest):
    basis, out = rest[:DEGREE], rest[DEGREE]
    total = jnp.sum(everyone[...], axis=0, keepdims=True)
    gram = {
        pair: jnp.broadcast_to(total[:, k : k + 1], (8, BLK)) for k, pair in enumerate(PAIRS)
    }
    substep = jnp.full((8, BLK), step[0] * 0.5, f32)
    one = jnp.ones((8, BLK), f32)
    forcing = [one] + [None] * DEGREE
    increment = [None] * (DEGREE + 1)
    for restart in range(2):
        start = forcing if restart == 0 else [add(x, y) for x, y in zip(jacobian(increment), forcing)]
        magnitude = jnp.sqrt(dot(start, through(gram, start)) + 1e-6)
        vectors = [scaled(start, 1.0 / magnitude)]
        hessenberg = [[None] * 3 for _ in range(3)]
        for j in range(3):
            mapped = jacobian(vectors[j])
            seen = through(gram, mapped)
            weights = [dot(v, seen) for v in vectors]
            for k, weight in enumerate(weights):
                hessenberg[k][j] = weight
            if j < 2:
                for v, weight in zip(vectors, weights):
                    mapped = [minus(x, times(y, weight)) for x, y in zip(mapped, v)]
                length = jnp.sqrt(dot(mapped, through(gram, mapped)) + 1e-6)
                hessenberg[j + 1][j] = length
                vectors.append(scaled(mapped, 1.0 / length))
        phi = phi_weights(hessenberg, substep)
        for v, weight in zip(vectors, phi):
            factor = substep * magnitude * weight
            increment = [add(x, times(y, factor)) for x, y in zip(increment, v)]
    for i in range(ROWS // 8):
        span = slice(8 * i, 8 * i + 8)
        line = concentration[span, :]
        for k in range(DEGREE):
            if increment[k] is not None:
                line = line + increment[k] * basis[k][span, :]
        out[span, :] = line


LIMIT = 16 << 20
FIELD = jax.ShapeDtypeStruct((ROWS, BLK), f32)
PACKETS = [jax.ShapeDtypeStruct((GHOST, BLK), f32)] * 4
PIECES = pltpu.VMEM((ROWS * BLK, 2 * BLK), bf16)
PARTIAL = [
    pltpu.VMEM((2 * GHOST + 8, BLK), f32),
    pltpu.VMEM((GROUP, BLK), f32),
] + [pltpu.VMEM((ROWS, BLK), f32)] * 4


def params():
    return pltpu.CompilerParams(vmem_limit_bytes=LIMIT)


def cost(flops):
    return pl.CostEstimate(flops=flops, bytes_accessed=0, transcendentals=0)


def hbm(n=1):
    return [pl.BlockSpec(memory_space=pltpu.HBM)] * n


def shards(pairs, concentration, rate, step, values, columns, lengths, send):
    devices = BLK

    def exchange(packets):
        arrived = []
        for t in range(4):
            arrived.append(lax.ppermute(packets[t], "dom", pairs[t]))
        return arrived

    send, concentration, rate, values, columns, lengths = (
        pltpu.with_memory_space_constraint(x, pltpu.HBM)
        for x in (send, concentration, rate, values.reshape(ENTRIES, BLK, BLK), columns.T, lengths)
    )
    concentration, rate, send, *packets = pl.pallas_call(
        first_packets,
        out_shape=[FIELD, FIELD, pltpu.SMEM((1, 4, GHOST), jnp.int32)] + PACKETS,
        in_specs=hbm(3),
        out_specs=vmem(2) + smem() + vmem(4),
        scratch_shapes=[pltpu.SemaphoreType.DMA((3,))],
        compiler_params=params(),
        name="first_packets",
    )(send, concentration, rate)
    arrived = exchange(packets)
    send = pltpu.with_memory_space_constraint(send, pltpu.SMEM)
    blocks, turned, table, near = pl.pallas_call(
        setup,
        out_shape=[
            pltpu.VMEM((ENTRIES, BLK, BLK), f32),
            pltpu.VMEM((BLK, BLK, 2 * BLK), bf16),
            pltpu.SMEM((TABLE,), jnp.int32),
            FIELD,
        ],
        in_specs=hbm(2) + smem() + hbm() + vmem(2),
        out_specs=vmem(2) + smem() + vmem(),
        scratch_shapes=[
            pltpu.SMEM((SLOTS, ROWS), jnp.int32),
            pltpu.SMEM((ROWS,), jnp.int32),
            PIECES,
            pltpu.SemaphoreType.DMA((CHUNKS,)),
            pltpu.SemaphoreType.DMA((2,)),
        ],
        compiler_params=params(),
        cost_estimate=cost(10**10),
        name="setup",
    )(columns, lengths, send, values, concentration, rate)
    blocks = pltpu.with_memory_space_constraint(blocks, pltpu.VMEM)
    turned = pltpu.with_memory_space_constraint(turned, pltpu.VMEM)
    table = pltpu.with_memory_space_constraint(table, pltpu.SMEM)
    basis = []

    def middle_call(near, arrived):
        return pl.pallas_call(
            middle_part,
            out_shape=FIELD,
            in_specs=smem() + vmem(4),
            out_specs=vmem()[0],
            scratch_shapes=PARTIAL,
            compiler_params=params(),
            cost_estimate=cost(10**9),
            name="middle_part",
        )(table, turned, near, *arrived[2:])

    near = middle_call(near, arrived)
    for k in range(DEGREE):
        field, *packets = pl.pallas_call(
            far_part(1.0 if k == 0 else SCALE),
            out_shape=[FIELD] + PACKETS,
            in_specs=smem() + vmem(4),
            out_specs=vmem(5),
            scratch_shapes=PARTIAL,
            compiler_params=params(),
            name="far_part",
        )(table, turned, near, *arrived[:2])
        basis.append(field)
        arrived = exchange(packets)
        near = pl.pallas_call(
            near_part,
            out_shape=FIELD,
            in_specs=smem() + vmem(4),
            out_specs=vmem()[0],
            scratch_shapes=[PIECES],
            compiler_params=params(),
            cost_estimate=cost(10**10),
            name="near_part",
        )(table, blocks, field, rate, concentration)
        near = middle_call(near, arrived)
    sums = pl.pallas_call(
        last_part,
        out_shape=jax.ShapeDtypeStruct((devices, BLK), f32),
        in_specs=smem() + vmem(4 + DEGREE),
        out_specs=vmem()[0],
        scratch_shapes=[pltpu.VMEM((ROWS, BLK), f32), pltpu.VMEM((BLK, BLK), f32)] + PARTIAL,
        compiler_params=params(),
        name="last_part",
    )(table, turned, near, *arrived[:2], *basis)
    everyone = lax.all_to_all(sums, "dom", split_axis=0, concat_axis=0, tiled=True)
    return pl.pallas_call(
        finish,
        out_shape=FIELD,
        in_specs=smem() + vmem(2 + DEGREE),
        out_specs=vmem()[0],
        compiler_params=params(),
        name="finish",
    )(step, everyone, concentration, *basis)


def solution(mesh):
    pairs = exchanges(mesh.shape["dom"])

    def run(*arrays):
        return shards(pairs, *arrays)

    split = P("dom")
    return jax.shard_map(
        run,
        mesh=mesh,
        in_specs=(split, split, P(), split, split, split, split),
        out_specs=split,
        check_vma=False,
    )
```

```python
import jax
import jax.numpy as jnp
from jax import lax
from jax.experimental import pallas as pl
from jax.experimental.pallas import tpu as pltpu
from jax.sharding import PartitionSpec as P

BLK = 128
ROWS = 32
SLOTS = 5
GHOST = 16
ENTRIES = ROWS * SLOTS
DEGREE = 6
SHIFT = 8.0
SCALE = 0.25
PAIRS = [(a, b) for b in range(DEGREE + 1) for a in range(min(b, DEGREE - 1) + 1)]

LIST = ENTRIES + 40
GROUPS = (40, 32, 32)
NEAR = 0
FAR = 3 * LIST
MID = 6 * LIST
REST = 9 * LIST
SEND = REST + 3 * LIST
COUNTS = SEND + 64
TABLE = COUNTS + 8
ZERO = ROWS

f32 = jnp.float32
bf16 = jnp.bfloat16


def vmem(n=1):
    return [pl.BlockSpec(memory_space=pltpu.VMEM)] * n


def smem(n=1):
    return [pl.BlockSpec(memory_space=pltpu.SMEM)] * n


def exchanges(devices):
    two = [(p, (p + 2) % devices) for p in range(devices)]
    one = [(p, (p + 1) % devices) for p in range(devices)]
    picked = (
        [e for e in two if e[0] % 4 >= 2],
        [e for e in one if e[0] % 2 == 1],
        [e for e in two if e[0] % 4 < 2],
        [e for e in one if e[0] % 2 == 0],
    )
    return [[(a, b) for a, b in es] + [(b, a) for a, b in es] for es in picked]


def roles():
    place = lax.axis_index("dom")
    even = (place % 2) == 0
    low = (place % 4) < 2
    pick = lambda c, a, b: jnp.where(c, jnp.int32(a), jnp.int32(b))
    return pick(low, 0, 3), pick(even, 1, 2), pick(low, 3, 0), pick(even, 2, 1)


def write_packets(field, row_of, packets):
    for t in range(4):
        for g in range(GHOST):
            packets[t][g : g + 1, :] = field[pl.ds(row_of(t, g), 1), :]


def first_packets(send, concentration, rate, field, speed, table, p0, p1, p2, p3, done):
    copies = [
        pltpu.make_async_copy(send, table, done.at[0]),
        pltpu.make_async_copy(concentration, field, done.at[1]),
        pltpu.make_async_copy(rate, speed, done.at[2]),
    ]
    for copy in copies:
        copy.start()
    by = roles()
    for copy in copies:
        copy.wait()
    write_packets(field, lambda t, g: table[0, by[t], g], (p0, p1, p2, p3))


def split(x):
    high = x.astype(bf16)
    return high, (x - high.astype(f32)).astype(bf16)


def setup(columns, lengths, send, values, field, rate, turned, table, out, where, length_of, blocks, done, small, *scratch):
    copies = [pltpu.make_async_copy(columns, where, small.at[0]), pltpu.make_async_copy(lengths, length_of, small.at[1])]
    for copy in copies:
        copy.start()

    def fetch(b):
        part = pl.ds(b * 2 * SLOTS, 2 * SLOTS)
        return pltpu.make_async_copy(values.at[part], blocks.at[part], done.at[b])

    for b in range(ROWS // 2):
        fetch(b).start()
    by = roles()
    place = lax.axis_index("dom")
    even = (place % 2) == 0
    low = (place % 4) < 2
    at = (
        jnp.where(low, 2, 0),
        jnp.where(even, 3, 1),
        jnp.where(even, 1, 3),
        jnp.where(low, 0, 2),
    )
    for t in range(4):
        for g in range(GHOST):
            table[SEND + t * GHOST + g] = send[0, by[t], g]
    for copy in copies:
        copy.wait()

    def rows(pair, carry):
        near, far, mid = carry
        fetch(pair).wait()
        for half in range(2):
            b = pair * 2 + half
            length = length_of[b]
            for s in range(SLOTS):
                column = where[s, b]
                index = jnp.maximum(column - ROWS, 0)
                q = index >> 4
                spot = jnp.where(q < 2, jnp.where(q == 0, at[0], at[1]), jnp.where(q == 2, at[2], at[3]))
                live = s < length
                ghost = jnp.logical_and(live, column >= ROWS)
                home = jnp.logical_and(live, column < ROWS)
                first = jnp.logical_and(ghost, spot < 2)
                second = jnp.logical_and(ghost, spot >= 2)
                base = jnp.where(
                    home, NEAR + near, jnp.where(first, FAR + far, jnp.where(second, MID + mid, REST))
                )
                table[base] = jnp.where(ghost, ((spot & 1) << 4) + (index & 15), column)
                table[base + LIST] = b * SLOTS + s
                table[base + 2 * LIST] = b
                near = near + home.astype(jnp.int32)
                far = far + first.astype(jnp.int32)
                mid = mid + second.astype(jnp.int32)
        for s in range(2 * SLOTS):
            slot = pair * 2 * SLOTS + s
            high, rest = split(jnp.transpose(blocks[slot]))
            turned[slot, :, 0:BLK] = high
            turned[slot, :, BLK : 2 * BLK] = rest
        return near, far, mid

    zero = jnp.int32(0)
    counts = lax.fori_loop(0, ROWS // 2, rows, (zero, zero, zero))
    for i, base in enumerate((NEAR, FAR, MID)):
        table[COUNTS + i] = counts[i]
        for g in range(GROUPS[i]):
            table[base + counts[i] + g] = ZERO
            table[base + LIST + counts[i] + g] = 0
            table[base + 2 * LIST + counts[i] + g] = 0
    total = product(table, 0, turned, (field,), *scratch)
    out[...] = rate[...] * field[...] * (1.0 - field[...]) - total


def near_part(table, turned, field, rate, concentration, out, *scratch):
    total = product(table, 0, turned, (field,), *scratch)
    slope = rate[...] * (1.0 - 2.0 * concentration[...]) + SHIFT
    out[...] = slope * field[...] - total


def product(table, which, turned, sources, lines, stage, *sums):
    base = (NEAR, FAR, MID)[which]
    size = GROUPS[which]
    count = table[COUNTS + which]
    height = ROWS // len(sources)
    for i, source in enumerate(sources):
        lines[i * height : (i + 1) * height, :] = source[...]
    lines[ZERO : ZERO + 8, :] = jnp.zeros((8, BLK), f32)
    for ref in sums:
        ref[...] = jnp.zeros((ROWS, BLK), f32)

    def group(c, carry):
        first = base + c * size
        for u in range(size):
            stage[u : u + 1, :] = lines[pl.ds(table[first + u], 1), :]
        for v in range(0, size, 8):
            left = jnp.concatenate(split(stage[v : v + 8, :]), axis=0)
            for u in range(v, v + 8):
                got = jnp.dot(left, turned[table[first + LIST + u]], preferred_element_type=f32)
                both = got[:, 0:BLK] + got[:, BLK : 2 * BLK]
                line = both[0:8] + both[8:16]
                to = pl.ds(table[first + 2 * LIST + u], 1)
                ref = sums[u % 4]
                ref[to, :] = ref[to, :] + line[u - v : u - v + 1, :]
        return carry

    lax.fori_loop(0, (count + size - 1) // size, group, 0)
    return (sums[0][...] + sums[1][...]) + (sums[2][...] + sums[3][...])


def middle_part(table, turned, near, g2, g3, out, *scratch):
    out[...] = near[...] - product(table, 2, turned, (g2, g3), *scratch)


def far_part(scale):
    def kernel(table, turned, near, g0, g1, out, p0, p1, p2, p3, *scratch):
        out[...] = (near[...] - product(table, 1, turned, (g0, g1), *scratch)) * scale
        write_packets(out, lambda t, g: table[SEND + t * GHOST + g], (p0, p1, p2, p3))

    return kernel


def last_part(table, turned, near, g0, g1, *rest):
    basis = rest[:DEGREE]
    sums, out, rows, *scratch = rest[DEGREE:]
    out[...] = (near[...] - product(table, 1, turned, (g0, g1), *scratch)) * SCALE
    basis = basis + (out,)
    rows[...] = jnp.zeros((BLK, BLK), f32)
    for k, (a, b) in enumerate(PAIRS):
        both = basis[a][...] * basis[b][...]
        rows[k : k + 1, :] = jnp.sum(both, axis=0, keepdims=True)
    line = lax.dot_general(
        jnp.ones((8, BLK), f32),
        rows[...],
        (((1,), (1,)), ((), ())),
        precision=lax.Precision.HIGHEST,
        preferred_element_type=f32,
    )
    sums[...] = jnp.broadcast_to(line[0:1], sums.shape)


def add(x, y):
    if x is None:
        return y
    return x if y is None else x + y


def times(x, y):
    return None if x is None or y is None else x * y


def minus(x, y):
    if y is None:
        return x
    return -y if x is None else x - y


def jacobian(v):
    out = [None if x is None else x * -SHIFT for x in v]
    for k in range(DEGREE):
        if v[k] is not None:
            out[k + 1] = add(out[k + 1], v[k] * (1.0 / SCALE))
    return out


def through(gram, v):
    return [
        (lambda terms: None if not terms else sum(terms[1:], terms[0]))(
            [gram[min(a, b), max(a, b)] * v[b] for b in range(DEGREE + 1) if v[b] is not None and (a, b) != (DEGREE, DEGREE)]
        )
        for a in range(DEGREE + 1)
    ]


def dot(u, v):
    terms = [x * y for x, y in zip(u, v) if x is not None and y is not None]
    return sum(terms[1:], terms[0])


def scaled(v, x):
    return [None if y is None else y * x for y in v]


def phi_weights(h, substep):
    n = len(h)
    reduced = [[None if x is None else x * substep * (1.0 / 64.0) for x in r] for r in h]
    matmul = lambda p, q: [
        [
            (lambda ts: None if not ts else sum(ts[1:], ts[0]))(
                [p[i][k] * q[k][j] for k in range(n) if p[i][k] is not None and q[k][j] is not None]
            )
            for j in range(n)
        ]
        for i in range(n)
    ]
    apply = lambda p, q: [
        (lambda ts: None if not ts else sum(ts[1:], ts[0]))(
            [p[i][k] * q[k] for k in range(n) if p[i][k] is not None and q[k] is not None]
        )
        for i in range(n)
    ]
    block = [[1.0 if i == j else None for j in range(n)] for i in range(n)]
    column = [None] * n
    for degree in range(12, 0, -1):
        inverse = 1.0 / degree
        block = matmul(reduced, block)
        block = [[None if x is None else x * inverse for x in r] for r in block]
        for i in range(n):
            block[i][i] = add(block[i][i], 1.0)
        column = apply(reduced, column)
        column[0] = add(column[0], 1.0 / 64.0)
        column = [None if x is None else x * inverse for x in column]
    for _ in range(6):
        moved = apply(block, column)
        column = [add(x, y) for x, y in zip(moved, column)]
        block = matmul(block, block)
    return column


def finish(step, everyone, concentration, *rest):
    basis, out = rest[:DEGREE], rest[DEGREE]
    total = jnp.sum(everyone[...], axis=0, keepdims=True)
    gram = {
        pair: jnp.broadcast_to(total[:, k : k + 1], (8, BLK)) for k, pair in enumerate(PAIRS)
    }
    substep = jnp.full((8, BLK), step[0] * 0.5, f32)
    one = jnp.ones((8, BLK), f32)
    forcing = [one] + [None] * DEGREE
    increment = [None] * (DEGREE + 1)
    for restart in range(2):
        start = forcing if restart == 0 else [add(x, y) for x, y in zip(jacobian(increment), forcing)]
        magnitude = jnp.sqrt(dot(start, through(gram, start)) + 1e-6)
        vectors = [scaled(start, 1.0 / magnitude)]
        hessenberg = [[None] * 3 for _ in range(3)]
        for j in range(3):
            mapped = jacobian(vectors[j])
            seen = through(gram, mapped)
            weights = [dot(v, seen) for v in vectors]
            for k, weight in enumerate(weights):
                hessenberg[k][j] = weight
            if j < 2:
                for v, weight in zip(vectors, weights):
                    mapped = [minus(x, times(y, weight)) for x, y in zip(mapped, v)]
                length = jnp.sqrt(dot(mapped, through(gram, mapped)) + 1e-6)
                hessenberg[j + 1][j] = length
                vectors.append(scaled(mapped, 1.0 / length))
        phi = phi_weights(hessenberg, substep)
        for v, weight in zip(vectors, phi):
            factor = substep * magnitude * weight
            increment = [add(x, times(y, factor)) for x, y in zip(increment, v)]
    for i in range(ROWS // 8):
        span = slice(8 * i, 8 * i + 8)
        line = concentration[span, :]
        for k in range(DEGREE):
            if increment[k] is not None:
                line = line + increment[k] * basis[k][span, :]
        out[span, :] = line


LIMIT = 24 << 20
FIELD = jax.ShapeDtypeStruct((ROWS, BLK), f32)
PACKETS = [jax.ShapeDtypeStruct((GHOST, BLK), f32)] * 4
PARTIAL = [
    pltpu.VMEM((ROWS + 8, BLK), f32),
    pltpu.VMEM((max(GROUPS), BLK), f32),
] + [pltpu.VMEM((ROWS, BLK), f32)] * 4


def params():
    return pltpu.CompilerParams(vmem_limit_bytes=LIMIT)


def cost(flops):
    return pl.CostEstimate(flops=flops, bytes_accessed=0, transcendentals=0)


def hbm(n=1):
    return [pl.BlockSpec(memory_space=pltpu.HBM)] * n


def shards(pairs, concentration, rate, step, values, columns, lengths, send):
    devices = BLK

    def exchange(packets):
        arrived = []
        for t in range(4):
            arrived.append(lax.ppermute(packets[t], "dom", pairs[t]))
        return arrived

    send, concentration, rate, values, columns, lengths = (
        pltpu.with_memory_space_constraint(x, pltpu.HBM)
        for x in (send, concentration, rate, values.reshape(ENTRIES, BLK, BLK), columns.T, lengths)
    )
    concentration, rate, send, *packets = pl.pallas_call(
        first_packets,
        out_shape=[FIELD, FIELD, pltpu.SMEM((1, 4, GHOST), jnp.int32)] + PACKETS,
        in_specs=hbm(3),
        out_specs=vmem(2) + smem() + vmem(4),
        scratch_shapes=[pltpu.SemaphoreType.DMA((3,))],
        compiler_params=params(),
        name="first_packets",
    )(send, concentration, rate)
    arrived = exchange(packets)
    send = pltpu.with_memory_space_constraint(send, pltpu.SMEM)
    turned, table, near = pl.pallas_call(
        setup,
        out_shape=[
            pltpu.VMEM((ENTRIES, BLK, 2 * BLK), bf16),
            pltpu.SMEM((TABLE,), jnp.int32),
            FIELD,
        ],
        in_specs=hbm(2) + smem() + hbm() + vmem(2),
        out_specs=vmem() + smem() + vmem(),
        scratch_shapes=[
            pltpu.SMEM((SLOTS, ROWS), jnp.int32),
            pltpu.SMEM((ROWS,), jnp.int32),
            pltpu.VMEM((ENTRIES, BLK, BLK), f32),
            pltpu.SemaphoreType.DMA((ROWS // 2,)),
            pltpu.SemaphoreType.DMA((2,)),
        ]
        + PARTIAL,
        compiler_params=params(),
        cost_estimate=cost(10**10),
        name="setup",
    )(columns, lengths, send, values, concentration, rate)
    turned = pltpu.with_memory_space_constraint(turned, pltpu.VMEM)
    table = pltpu.with_memory_space_constraint(table, pltpu.SMEM)
    basis = []

    def middle_call(near, arrived):
        return pl.pallas_call(
            middle_part,
            out_shape=FIELD,
            in_specs=smem() + vmem(4),
            out_specs=vmem()[0],
            scratch_shapes=PARTIAL,
            compiler_params=params(),
            cost_estimate=cost(10**9),
            name="middle_part",
        )(table, turned, near, *arrived[2:])

    near = middle_call(near, arrived)
    for k in range(DEGREE):
        field, *packets = pl.pallas_call(
            far_part(1.0 if k == 0 else SCALE),
            out_shape=[FIELD] + PACKETS,
            in_specs=smem() + vmem(4),
            out_specs=vmem(5),
            scratch_shapes=PARTIAL,
            compiler_params=params(),
            name="far_part",
        )(table, turned, near, *arrived[:2])
        basis.append(field)
        arrived = exchange(packets)
        near = pl.pallas_call(
            near_part,
            out_shape=FIELD,
            in_specs=smem() + vmem(4),
            out_specs=vmem()[0],
            scratch_shapes=PARTIAL,
            compiler_params=params(),
            cost_estimate=cost(10**10),
            name="near_part",
        )(table, turned, field, rate, concentration)
        near = middle_call(near, arrived)
    sums = pl.pallas_call(
        last_part,
        out_shape=jax.ShapeDtypeStruct((devices, BLK), f32),
        in_specs=smem() + vmem(4 + DEGREE),
        out_specs=vmem()[0],
        scratch_shapes=[pltpu.VMEM((ROWS, BLK), f32), pltpu.VMEM((BLK, BLK), f32)] + PARTIAL,
        compiler_params=params(),
        name="last_part",
    )(table, turned, near, *arrived[:2], *basis)
    everyone = lax.all_to_all(sums, "dom", split_axis=0, concat_axis=0, tiled=True)
    return pl.pallas_call(
        finish,
        out_shape=FIELD,
        in_specs=smem() + vmem(2 + DEGREE),
        out_specs=vmem()[0],
        compiler_params=params(),
        name="finish",
    )(step, everyone, concentration, *basis)


def solution(mesh):
    pairs = exchanges(mesh.shape["dom"])

    def run(*arrays):
        return shards(pairs, *arrays)

    split = P("dom")
    return jax.shard_map(
        run,
        mesh=mesh,
        in_specs=(split, split, P(), split, split, split, split),
        out_specs=split,
        check_vma=False,
    )
```

```python
import jax
import jax.numpy as jnp
from jax import lax
from jax.experimental import pallas as pl
from jax.experimental.pallas import tpu as pltpu
from jax.sharding import PartitionSpec as P

BLK = 128
ROWS = 32
SLOTS = 5
GHOST = 16
ENTRIES = ROWS * SLOTS
DEGREE = 6
SHIFT = 8.0
SCALE = 0.25
PAIRS = [(a, b) for b in range(DEGREE + 1) for a in range(min(b, DEGREE - 1) + 1)]

GROUPS = (80, 56)
LIST = ENTRIES + max(GROUPS)
NEAR = 0
FAR = 3 * LIST
REST = 6 * LIST
SEND = REST + 3 * LIST
COUNTS = SEND + 64
TABLE = COUNTS + 8
LINES = 4 * GHOST

f32 = jnp.float32
bf16 = jnp.bfloat16


def vmem(n=1):
    return [pl.BlockSpec(memory_space=pltpu.VMEM)] * n


def smem(n=1):
    return [pl.BlockSpec(memory_space=pltpu.SMEM)] * n


def exchanges(devices):
    two = [(p, (p + 2) % devices) for p in range(devices)]
    one = [(p, (p + 1) % devices) for p in range(devices)]
    picked = (
        [e for e in two if e[0] % 4 >= 2],
        [e for e in one if e[0] % 2 == 1],
        [e for e in two if e[0] % 4 < 2],
        [e for e in one if e[0] % 2 == 0],
    )
    return [[(a, b) for a, b in es] + [(b, a) for a, b in es] for es in picked]


def roles():
    place = lax.axis_index("dom")
    even = (place % 2) == 0
    low = (place % 4) < 2
    pick = lambda c, a, b: jnp.where(c, jnp.int32(a), jnp.int32(b))
    return pick(low, 0, 3), pick(even, 1, 2), pick(low, 3, 0), pick(even, 2, 1)


def write_packets(field, row_of, packets):
    for t in range(4):
        for g in range(GHOST):
            packets[t][g : g + 1, :] = field[pl.ds(row_of(t, g), 1), :]


def first_packets(send, concentration, rate, field, speed, table, p0, p1, p2, p3, done):
    copies = [
        pltpu.make_async_copy(send, table, done.at[0]),
        pltpu.make_async_copy(concentration, field, done.at[1]),
        pltpu.make_async_copy(rate, speed, done.at[2]),
    ]
    for copy in copies:
        copy.start()
    by = roles()
    for copy in copies:
        copy.wait()
    write_packets(field, lambda t, g: table[0, by[t], g], (p0, p1, p2, p3))


def split(x):
    high = x.astype(bf16)
    return high, (x - high.astype(f32)).astype(bf16)


def setup(columns, lengths, send, values, field, rate, turned, table, out, where, length_of, blocks, done, small, *scratch):
    copies = [pltpu.make_async_copy(columns, where, small.at[0]), pltpu.make_async_copy(lengths, length_of, small.at[1])]
    for copy in copies:
        copy.start()

    def fetch(b):
        part = pl.ds(b * 2 * SLOTS, 2 * SLOTS)
        return pltpu.make_async_copy(values.at[part], blocks.at[part], done.at[b])

    for b in range(ROWS // 2):
        fetch(b).start()
    by = roles()
    place = lax.axis_index("dom")
    even = (place % 2) == 0
    low = (place % 4) < 2
    at = (
        jnp.where(low, 2, 0),
        jnp.where(even, 3, 1),
        jnp.where(even, 1, 3),
        jnp.where(low, 0, 2),
    )
    for t in range(4):
        for g in range(GHOST):
            table[SEND + t * GHOST + g] = send[0, by[t], g]
    for copy in copies:
        copy.wait()

    def rows(pair, carry):
        near, far = carry
        fetch(pair).wait()
        for half in range(2):
            b = pair * 2 + half
            length = length_of[b]
            for s in range(SLOTS):
                column = where[s, b]
                index = jnp.maximum(column - ROWS, 0)
                q = index >> 4
                spot = jnp.where(q < 2, jnp.where(q == 0, at[0], at[1]), jnp.where(q == 2, at[2], at[3]))
                live = s < length
                ghost = jnp.logical_and(live, column >= ROWS)
                home = jnp.logical_and(live, column < ROWS)
                base = jnp.where(home, NEAR + near, jnp.where(ghost, FAR + far, REST))
                table[base] = jnp.where(ghost, (spot << 4) + (index & 15), column)
                table[base + LIST] = b * SLOTS + s
                table[base + 2 * LIST] = b
                near = near + home.astype(jnp.int32)
                far = far + ghost.astype(jnp.int32)
        for s in range(2 * SLOTS):
            slot = pair * 2 * SLOTS + s
            high, rest = split(jnp.transpose(blocks[slot]))
            turned[slot, :, 0:BLK] = high
            turned[slot, :, BLK : 2 * BLK] = rest
        return near, far

    zero = jnp.int32(0)
    counts = lax.fori_loop(0, ROWS // 2, rows, (zero, zero))
    for i, base in enumerate((NEAR, FAR)):
        table[COUNTS + i] = counts[i]
        for g in range(GROUPS[i]):
            table[base + counts[i] + g] = LINES
            table[base + LIST + counts[i] + g] = 0
            table[base + 2 * LIST + counts[i] + g] = 0
    total = product(table, 0, turned, (field,), *scratch)
    out[...] = rate[...] * field[...] * (1.0 - field[...]) - total


def near_part(table, turned, field, rate, concentration, out, *scratch):
    total = product(table, 0, turned, (field,), *scratch)
    slope = rate[...] * (1.0 - 2.0 * concentration[...]) + SHIFT
    out[...] = slope * field[...] - total


def product(table, which, turned, sources, lines, stage, *sums):
    base = (NEAR, FAR)[which]
    size = GROUPS[which]
    count = table[COUNTS + which]
    for i, source in enumerate(sources):
        height = source.shape[0]
        lines[i * height : (i + 1) * height, :] = source[...]
    lines[LINES : LINES + 8, :] = jnp.zeros((8, BLK), f32)
    for ref in sums:
        ref[...] = jnp.zeros((ROWS, BLK), f32)

    def group(c, carry):
        first = base + c * size
        for u in range(size):
            stage[u : u + 1, :] = lines[pl.ds(table[first + u], 1), :]
        for v in range(0, size, 8):
            left = jnp.concatenate(split(stage[v : v + 8, :]), axis=0)
            for u in range(v, v + 8):
                got = jnp.dot(left, turned[table[first + LIST + u]], preferred_element_type=f32)
                both = got[:, 0:BLK] + got[:, BLK : 2 * BLK]
                line = both[0:8] + both[8:16]
                to = pl.ds(table[first + 2 * LIST + u], 1)
                ref = sums[u % 4]
                ref[to, :] = ref[to, :] + line[u - v : u - v + 1, :]
        return carry

    lax.fori_loop(0, (count + size - 1) // size, group, 0)
    return (sums[0][...] + sums[1][...]) + (sums[2][...] + sums[3][...])


def far_part(scale):
    def kernel(table, turned, near, g0, g1, g2, g3, out, p0, p1, p2, p3, *scratch):
        out[...] = (near[...] - product(table, 1, turned, (g0, g1, g2, g3), *scratch)) * scale
        write_packets(out, lambda t, g: table[SEND + t * GHOST + g], (p0, p1, p2, p3))

    return kernel


def last_part(table, turned, near, g0, g1, g2, g3, *rest):
    basis = rest[:DEGREE]
    sums, out, rows, *scratch = rest[DEGREE:]
    out[...] = (near[...] - product(table, 1, turned, (g0, g1, g2, g3), *scratch)) * SCALE
    basis = basis + (out,)
    rows[...] = jnp.zeros(rows.shape, f32)
    for k, (a, b) in enumerate(PAIRS):
        both = basis[a][...] * basis[b][...]
        rows[k : k + 1, :] = jnp.sum(both, axis=0, keepdims=True)
    line = jnp.sum(jnp.transpose(rows[...]), axis=0, keepdims=True)
    sums[...] = jnp.broadcast_to(line, sums.shape)


def add(x, y):
    if x is None:
        return y
    return x if y is None else x + y


def times(x, y):
    return None if x is None or y is None else x * y


def minus(x, y):
    if y is None:
        return x
    return -y if x is None else x - y


def jacobian(v):
    out = [None if x is None else x * -SHIFT for x in v]
    for k in range(DEGREE):
        if v[k] is not None:
            out[k + 1] = add(out[k + 1], v[k] * (1.0 / SCALE))
    return out


def through(gram, v):
    return [
        (lambda terms: None if not terms else sum(terms[1:], terms[0]))(
            [gram[min(a, b), max(a, b)] * v[b] for b in range(DEGREE + 1) if v[b] is not None and (a, b) != (DEGREE, DEGREE)]
        )
        for a in range(DEGREE + 1)
    ]


def dot(u, v):
    terms = [x * y for x, y in zip(u, v) if x is not None and y is not None]
    return sum(terms[1:], terms[0])


def scaled(v, x):
    return [None if y is None else y * x for y in v]


def phi_weights(h, substep):
    n = len(h)
    reduced = [[None if x is None else x * substep * (1.0 / 64.0) for x in r] for r in h]
    matmul = lambda p, q: [
        [
            (lambda ts: None if not ts else sum(ts[1:], ts[0]))(
                [p[i][k] * q[k][j] for k in range(n) if p[i][k] is not None and q[k][j] is not None]
            )
            for j in range(n)
        ]
        for i in range(n)
    ]
    apply = lambda p, q: [
        (lambda ts: None if not ts else sum(ts[1:], ts[0]))(
            [p[i][k] * q[k] for k in range(n) if p[i][k] is not None and q[k] is not None]
        )
        for i in range(n)
    ]
    block = [[1.0 if i == j else None for j in range(n)] for i in range(n)]
    column = [None] * n
    for degree in range(12, 0, -1):
        inverse = 1.0 / degree
        block = matmul(reduced, block)
        block = [[None if x is None else x * inverse for x in r] for r in block]
        for i in range(n):
            block[i][i] = add(block[i][i], 1.0)
        column = apply(reduced, column)
        column[0] = add(column[0], 1.0 / 64.0)
        column = [None if x is None else x * inverse for x in column]
    for _ in range(6):
        moved = apply(block, column)
        column = [add(x, y) for x, y in zip(moved, column)]
        block = matmul(block, block)
    return column


def finish(step, everyone, concentration, *rest):
    basis, out = rest[:DEGREE], rest[DEGREE]
    total = jnp.sum(everyone[...], axis=0, keepdims=True)
    gram = {
        pair: jnp.broadcast_to(total[:, k : k + 1], (8, BLK)) for k, pair in enumerate(PAIRS)
    }
    substep = jnp.full((8, BLK), step[0] * 0.5, f32)
    one = jnp.ones((8, BLK), f32)
    forcing = [one] + [None] * DEGREE
    increment = [None] * (DEGREE + 1)
    for restart in range(2):
        start = forcing if restart == 0 else [add(x, y) for x, y in zip(jacobian(increment), forcing)]
        magnitude = jnp.sqrt(dot(start, through(gram, start)) + 1e-6)
        vectors = [scaled(start, 1.0 / magnitude)]
        hessenberg = [[None] * 3 for _ in range(3)]
        for j in range(3):
            mapped = jacobian(vectors[j])
            seen = through(gram, mapped)
            weights = [dot(v, seen) for v in vectors]
            for k, weight in enumerate(weights):
                hessenberg[k][j] = weight
            if j < 2:
                for v, weight in zip(vectors, weights):
                    mapped = [minus(x, times(y, weight)) for x, y in zip(mapped, v)]
                length = jnp.sqrt(dot(mapped, through(gram, mapped)) + 1e-6)
                hessenberg[j + 1][j] = length
                vectors.append(scaled(mapped, 1.0 / length))
        phi = phi_weights(hessenberg, substep)
        for v, weight in zip(vectors, phi):
            factor = substep * magnitude * weight
            increment = [add(x, times(y, factor)) for x, y in zip(increment, v)]
    for i in range(ROWS // 8):
        span = slice(8 * i, 8 * i + 8)
        line = concentration[span, :]
        for k in range(DEGREE):
            if increment[k] is not None:
                line = line + increment[k] * basis[k][span, :]
        out[span, :] = line


LIMIT = 24 << 20
FIELD = jax.ShapeDtypeStruct((ROWS, BLK), f32)
PACKETS = [jax.ShapeDtypeStruct((GHOST, BLK), f32)] * 4
PARTIAL = [
    pltpu.VMEM((LINES + 8, BLK), f32),
    pltpu.VMEM((max(GROUPS), BLK), f32),
] + [pltpu.VMEM((ROWS, BLK), f32)] * 4


def params():
    return pltpu.CompilerParams(vmem_limit_bytes=LIMIT)


def cost(flops):
    return pl.CostEstimate(flops=flops, bytes_accessed=0, transcendentals=0)


def hbm(n=1):
    return [pl.BlockSpec(memory_space=pltpu.HBM)] * n


def shards(pairs, concentration, rate, step, values, columns, lengths, send):
    devices = BLK

    def exchange(packets):
        arrived = []
        for t in range(4):
            arrived.append(lax.ppermute(packets[t], "dom", pairs[t]))
        return arrived

    send, concentration, rate, values, columns, lengths = (
        pltpu.with_memory_space_constraint(x, pltpu.HBM)
        for x in (send, concentration, rate, values.reshape(ENTRIES, BLK, BLK), columns.T, lengths)
    )
    concentration, rate, send, *packets = pl.pallas_call(
        first_packets,
        out_shape=[FIELD, FIELD, pltpu.SMEM((1, 4, GHOST), jnp.int32)] + PACKETS,
        in_specs=hbm(3),
        out_specs=vmem(2) + smem() + vmem(4),
        scratch_shapes=[pltpu.SemaphoreType.DMA((3,))],
        compiler_params=params(),
        name="first_packets",
    )(send, concentration, rate)
    arrived = exchange(packets)
    send = pltpu.with_memory_space_constraint(send, pltpu.SMEM)
    turned, table, near = pl.pallas_call(
        setup,
        out_shape=[
            pltpu.VMEM((ENTRIES, BLK, 2 * BLK), bf16),
            pltpu.SMEM((TABLE,), jnp.int32),
            FIELD,
        ],
        in_specs=hbm(2) + smem() + hbm() + vmem(2),
        out_specs=vmem() + smem() + vmem(),
        scratch_shapes=[
            pltpu.SMEM((SLOTS, ROWS), jnp.int32),
            pltpu.SMEM((ROWS,), jnp.int32),
            pltpu.VMEM((ENTRIES, BLK, BLK), f32),
            pltpu.SemaphoreType.DMA((ROWS // 2,)),
            pltpu.SemaphoreType.DMA((2,)),
        ]
        + PARTIAL,
        compiler_params=params(),
        cost_estimate=cost(10**10),
        name="setup",
    )(columns, lengths, send, values, concentration, rate)
    turned = pltpu.with_memory_space_constraint(turned, pltpu.VMEM)
    table = pltpu.with_memory_space_constraint(table, pltpu.SMEM)
    basis = []

    for k in range(DEGREE):
        field, *packets = pl.pallas_call(
            far_part(1.0 if k == 0 else SCALE),
            out_shape=[FIELD] + PACKETS,
            in_specs=smem() + vmem(6),
            out_specs=vmem(5),
            scratch_shapes=PARTIAL,
            compiler_params=params(),
            name="far_part",
        )(table, turned, near, *arrived)
        basis.append(field)
        arrived = exchange(packets)
        near = pl.pallas_call(
            near_part,
            out_shape=FIELD,
            in_specs=smem() + vmem(4),
            out_specs=vmem()[0],
            scratch_shapes=PARTIAL,
            compiler_params=params(),
            cost_estimate=cost(10**10),
            name="near_part",
        )(table, turned, field, rate, concentration)
    sums = pl.pallas_call(
        last_part,
        out_shape=jax.ShapeDtypeStruct((devices, ROWS), f32),
        in_specs=smem() + vmem(6 + DEGREE),
        out_specs=vmem()[0],
        scratch_shapes=[pltpu.VMEM((ROWS, BLK), f32), pltpu.VMEM((ROWS, BLK), f32)] + PARTIAL,
        compiler_params=params(),
        name="last_part",
    )(table, turned, near, *arrived, *basis)
    everyone = lax.all_to_all(sums, "dom", split_axis=0, concat_axis=0, tiled=True)
    return pl.pallas_call(
        finish,
        out_shape=FIELD,
        in_specs=smem() + vmem(2 + DEGREE),
        out_specs=vmem()[0],
        compiler_params=params(),
        name="finish",
    )(step, everyone, concentration, *basis)


def solution(mesh):
    pairs = exchanges(mesh.shape["dom"])

    def run(*arrays):
        return shards(pairs, *arrays)

    split = P("dom")
    return jax.shard_map(
        run,
        mesh=mesh,
        in_specs=(split, split, P(), split, split, split, split),
        out_specs=split,
        check_vma=False,
    )
```

```python
import jax
import jax.numpy as jnp
from jax import lax
from jax.experimental import pallas as pl
from jax.experimental.pallas import tpu as pltpu
from jax.sharding import PartitionSpec as P

BLK = 128
ROWS = 32
SLOTS = 5
GHOST = 16
ENTRIES = ROWS * SLOTS
DEGREE = 6
SHIFT = 8.0
SCALE = 0.25
PAIRS = [(a, b) for b in range(DEGREE + 1) for a in range(min(b, DEGREE - 1) + 1)]

GROUPS = (80, 56)
LIST = ENTRIES + max(GROUPS)
NEAR = 0
FAR = 3 * LIST
REST = 6 * LIST
SEND = REST + 3 * LIST
COUNTS = SEND + 64
TABLE = COUNTS + 8
LINES = 4 * GHOST

FIRST_OFFSETS = (1, 2, -2, -1)
FIRST_INDICES = (2, 3, 0, 1)

f32 = jnp.float32
bf16 = jnp.bfloat16


def vmem(n=1):
    return [pl.BlockSpec(memory_space=pltpu.VMEM)] * n


def smem(n=1):
    return [pl.BlockSpec(memory_space=pltpu.SMEM)] * n


def exchanges(devices):
    two = [(p, (p + 2) % devices) for p in range(devices)]
    one = [(p, (p + 1) % devices) for p in range(devices)]
    picked = (
        [e for e in two if e[0] % 4 >= 2],
        [e for e in one if e[0] % 2 == 1],
        [e for e in two if e[0] % 4 < 2],
        [e for e in one if e[0] % 2 == 0],
    )
    both = [es + [(b, a) for a, b in es] for es in picked]
    shifts = [[(p, (p + o) % devices) for p in range(devices)] for o in FIRST_OFFSETS]
    return shifts, both


def places():
    place = lax.axis_index("dom")
    even = (place % 2) == 0
    low = (place % 4) < 2
    return jnp.where(low, 2, 0), jnp.where(even, 3, 1), jnp.where(even, 1, 3), jnp.where(low, 0, 2)


def roles():
    place = lax.axis_index("dom")
    even = (place % 2) == 0
    low = (place % 4) < 2
    pick = lambda c, a, b: jnp.where(c, jnp.int32(a), jnp.int32(b))
    return pick(low, 0, 3), pick(even, 1, 2), pick(low, 3, 0), pick(even, 2, 1)


def write_packets(field, row_of, packets):
    for t in range(4):
        for g in range(GHOST):
            packets[t][g : g + 1, :] = field[pl.ds(row_of(t, g), 1), :]


def first_packets(send, concentration, rate, field, speed, table, p0, p1, p2, p3, done):
    copies = [
        pltpu.make_async_copy(send, table, done.at[0]),
        pltpu.make_async_copy(concentration, field, done.at[1]),
        pltpu.make_async_copy(rate, speed, done.at[2]),
    ]
    for copy in copies:
        copy.start()
    for copy in copies:
        copy.wait()
    write_packets(field, lambda t, g: table[0, FIRST_INDICES[t], g], (p0, p1, p2, p3))


def split(x):
    high = x.astype(bf16)
    return high, (x - high.astype(f32)).astype(bf16)


def setup(columns, lengths, send, values, field, rate, turned, table, out, where, length_of, blocks, done, small, *scratch):
    copies = [pltpu.make_async_copy(columns, where, small.at[0]), pltpu.make_async_copy(lengths, length_of, small.at[1])]
    for copy in copies:
        copy.start()

    def fetch(b):
        part = pl.ds(b * 2 * SLOTS, 2 * SLOTS)
        return pltpu.make_async_copy(values.at[part], blocks.at[part], done.at[b])

    for b in range(ROWS // 2):
        fetch(b).start()
    by = roles()
    at = places()
    for t in range(4):
        for g in range(GHOST):
            table[SEND + t * GHOST + g] = send[0, by[t], g]
    for copy in copies:
        copy.wait()

    def rows(pair, carry):
        near, far = carry
        fetch(pair).wait()
        for half in range(2):
            b = pair * 2 + half
            length = length_of[b]
            for s in range(SLOTS):
                column = where[s, b]
                index = jnp.maximum(column - ROWS, 0)
                q = index >> 4
                spot = jnp.where(q < 2, jnp.where(q == 0, at[0], at[1]), jnp.where(q == 2, at[2], at[3]))
                live = s < length
                ghost = jnp.logical_and(live, column >= ROWS)
                home = jnp.logical_and(live, column < ROWS)
                base = jnp.where(home, NEAR + near, jnp.where(ghost, FAR + far, REST))
                table[base] = jnp.where(ghost, (spot << 4) + (index & 15), column)
                table[base + LIST] = b * SLOTS + s
                table[base + 2 * LIST] = b
                near = near + home.astype(jnp.int32)
                far = far + ghost.astype(jnp.int32)
        for s in range(2 * SLOTS):
            slot = pair * 2 * SLOTS + s
            high, rest = split(jnp.transpose(blocks[slot]))
            turned[slot, :, 0:BLK] = high
            turned[slot, :, BLK : 2 * BLK] = rest
        return near, far

    zero = jnp.int32(0)
    counts = lax.fori_loop(0, ROWS // 2, rows, (zero, zero))
    for i, base in enumerate((NEAR, FAR)):
        table[COUNTS + i] = counts[i]
        for g in range(GROUPS[i]):
            table[base + counts[i] + g] = LINES
            table[base + LIST + counts[i] + g] = 0
            table[base + 2 * LIST + counts[i] + g] = 0
    total = product(table, 0, turned, (field,), *scratch)
    out[...] = rate[...] * field[...] * (1.0 - field[...]) - total


def near_part(table, turned, field, rate, concentration, out, *scratch):
    total = product(table, 0, turned, (field,), *scratch)
    slope = rate[...] * (1.0 - 2.0 * concentration[...]) + SHIFT
    out[...] = slope * field[...] - total


def product(table, which, turned, sources, lines, stage, *sums, order=None):
    base = (NEAR, FAR)[which]
    size = GROUPS[which]
    count = table[COUNTS + which]
    for i, source in enumerate(sources):
        height = source.shape[0]
        start = i * height if order is None else pl.multiple_of(order[i] * height, height)
        lines[pl.ds(start, height), :] = source[...]
    lines[LINES : LINES + 8, :] = jnp.zeros((8, BLK), f32)
    for ref in sums:
        ref[...] = jnp.zeros((ROWS, BLK), f32)

    def group(c, carry):
        first = base + c * size
        for u in range(size):
            stage[u : u + 1, :] = lines[pl.ds(table[first + u], 1), :]
        for v in range(0, size, 8):
            left = jnp.concatenate(split(stage[v : v + 8, :]), axis=0)
            for u in range(v, v + 8):
                got = jnp.dot(left, turned[table[first + LIST + u]], preferred_element_type=f32)
                both = got[:, 0:BLK] + got[:, BLK : 2 * BLK]
                line = both[0:8] + both[8:16]
                to = pl.ds(table[first + 2 * LIST + u], 1)
                ref = sums[u % 4]
                ref[to, :] = ref[to, :] + line[u - v : u - v + 1, :]
        return carry

    lax.fori_loop(0, (count + size - 1) // size, group, 0)
    return (sums[0][...] + sums[1][...]) + (sums[2][...] + sums[3][...])


def far_part(first):
    def kernel(table, turned, near, g0, g1, g2, g3, out, p0, p1, p2, p3, *scratch):
        at = places()
        order = [at[q] for q in FIRST_INDICES] if first else None
        total = product(table, 1, turned, (g0, g1, g2, g3), *scratch, order=order)
        out[...] = (near[...] - total) * (1.0 if first else SCALE)
        write_packets(out, lambda t, g: table[SEND + t * GHOST + g], (p0, p1, p2, p3))

    return kernel


def last_part(table, turned, near, g0, g1, g2, g3, *rest):
    basis = rest[:DEGREE]
    sums, out, rows, *scratch = rest[DEGREE:]
    out[...] = (near[...] - product(table, 1, turned, (g0, g1, g2, g3), *scratch)) * SCALE
    basis = basis + (out,)
    rows[...] = jnp.zeros(rows.shape, f32)
    for k, (a, b) in enumerate(PAIRS):
        both = basis[a][...] * basis[b][...]
        rows[k : k + 1, :] = jnp.sum(both, axis=0, keepdims=True)
    line = jnp.sum(jnp.transpose(rows[...]), axis=0, keepdims=True)
    sums[...] = jnp.broadcast_to(line, sums.shape)


def add(x, y):
    if x is None:
        return y
    return x if y is None else x + y


def times(x, y):
    return None if x is None or y is None else x * y


def minus(x, y):
    if y is None:
        return x
    return -y if x is None else x - y


def jacobian(v):
    out = [None if x is None else x * -SHIFT for x in v]
    for k in range(DEGREE):
        if v[k] is not None:
            out[k + 1] = add(out[k + 1], v[k] * (1.0 / SCALE))
    return out


def through(gram, v):
    return [
        (lambda terms: None if not terms else sum(terms[1:], terms[0]))(
            [gram[min(a, b), max(a, b)] * v[b] for b in range(DEGREE + 1) if v[b] is not None and (a, b) != (DEGREE, DEGREE)]
        )
        for a in range(DEGREE + 1)
    ]


def dot(u, v):
    terms = [x * y for x, y in zip(u, v) if x is not None and y is not None]
    return sum(terms[1:], terms[0])


def scaled(v, x):
    return [None if y is None else y * x for y in v]


def phi_weights(h, substep):
    n = len(h)
    reduced = [[None if x is None else x * substep * (1.0 / 64.0) for x in r] for r in h]
    matmul = lambda p, q: [
        [
            (lambda ts: None if not ts else sum(ts[1:], ts[0]))(
                [p[i][k] * q[k][j] for k in range(n) if p[i][k] is not None and q[k][j] is not None]
            )
            for j in range(n)
        ]
        for i in range(n)
    ]
    apply = lambda p, q: [
        (lambda ts: None if not ts else sum(ts[1:], ts[0]))(
            [p[i][k] * q[k] for k in range(n) if p[i][k] is not None and q[k] is not None]
        )
        for i in range(n)
    ]
    block = [[1.0 if i == j else None for j in range(n)] for i in range(n)]
    column = [None] * n
    for degree in range(12, 0, -1):
        inverse = 1.0 / degree
        block = matmul(reduced, block)
        block = [[None if x is None else x * inverse for x in r] for r in block]
        for i in range(n):
            block[i][i] = add(block[i][i], 1.0)
        column = apply(reduced, column)
        column[0] = add(column[0], 1.0 / 64.0)
        column = [None if x is None else x * inverse for x in column]
    for _ in range(6):
        moved = apply(block, column)
        column = [add(x, y) for x, y in zip(moved, column)]
        block = matmul(block, block)
    return column


def finish(step, everyone, concentration, *rest):
    basis, out = rest[:DEGREE], rest[DEGREE]
    total = jnp.sum(everyone[...], axis=0, keepdims=True)
    gram = {
        pair: jnp.broadcast_to(total[:, k : k + 1], (8, BLK)) for k, pair in enumerate(PAIRS)
    }
    substep = jnp.full((8, BLK), step[0] * 0.5, f32)
    one = jnp.ones((8, BLK), f32)
    forcing = [one] + [None] * DEGREE
    increment = [None] * (DEGREE + 1)
    for restart in range(2):
        start = forcing if restart == 0 else [add(x, y) for x, y in zip(jacobian(increment), forcing)]
        magnitude = jnp.sqrt(dot(start, through(gram, start)) + 1e-6)
        vectors = [scaled(start, 1.0 / magnitude)]
        hessenberg = [[None] * 3 for _ in range(3)]
        for j in range(3):
            mapped = jacobian(vectors[j])
            seen = through(gram, mapped)
            weights = [dot(v, seen) for v in vectors]
            for k, weight in enumerate(weights):
                hessenberg[k][j] = weight
            if j < 2:
                for v, weight in zip(vectors, weights):
                    mapped = [minus(x, times(y, weight)) for x, y in zip(mapped, v)]
                length = jnp.sqrt(dot(mapped, through(gram, mapped)) + 1e-6)
                hessenberg[j + 1][j] = length
                vectors.append(scaled(mapped, 1.0 / length))
        phi = phi_weights(hessenberg, substep)
        for v, weight in zip(vectors, phi):
            factor = substep * magnitude * weight
            increment = [add(x, times(y, factor)) for x, y in zip(increment, v)]
    for i in range(ROWS // 8):
        span = slice(8 * i, 8 * i + 8)
        line = concentration[span, :]
        for k in range(DEGREE):
            if increment[k] is not None:
                line = line + increment[k] * basis[k][span, :]
        out[span, :] = line


LIMIT = 24 << 20
FIELD = jax.ShapeDtypeStruct((ROWS, BLK), f32)
PACKETS = [jax.ShapeDtypeStruct((GHOST, BLK), f32)] * 4
PARTIAL = [
    pltpu.VMEM((LINES + 8, BLK), f32),
    pltpu.VMEM((max(GROUPS), BLK), f32),
] + [pltpu.VMEM((ROWS, BLK), f32)] * 4


def params():
    return pltpu.CompilerParams(vmem_limit_bytes=LIMIT)


def cost(flops):
    return pl.CostEstimate(flops=flops, bytes_accessed=0, transcendentals=0)


def hbm(n=1):
    return [pl.BlockSpec(memory_space=pltpu.HBM)] * n


def shards(shifts, swaps, concentration, rate, step, values, columns, lengths, send):
    devices = BLK

    def exchange(packets, k):
        arrived = []
        for t in range(4):
            arrived.append(lax.ppermute(packets[t], "dom", (swaps if k else shifts)[t]))
        return arrived

    send, concentration, rate, values, columns, lengths = (
        pltpu.with_memory_space_constraint(x, pltpu.HBM)
        for x in (send, concentration, rate, values.reshape(ENTRIES, BLK, BLK), columns.T, lengths)
    )
    concentration, rate, send, *packets = pl.pallas_call(
        first_packets,
        out_shape=[FIELD, FIELD, pltpu.SMEM((1, 4, GHOST), jnp.int32)] + PACKETS,
        in_specs=hbm(3),
        out_specs=vmem(2) + smem() + vmem(4),
        scratch_shapes=[pltpu.SemaphoreType.DMA((3,))],
        compiler_params=params(),
        name="first_packets",
    )(send, concentration, rate)
    arrived = exchange(packets, 0)
    send = pltpu.with_memory_space_constraint(send, pltpu.SMEM)
    turned, table, near = pl.pallas_call(
        setup,
        out_shape=[
            pltpu.VMEM((ENTRIES, BLK, 2 * BLK), bf16),
            pltpu.SMEM((TABLE,), jnp.int32),
            FIELD,
        ],
        in_specs=hbm(2) + smem() + hbm() + vmem(2),
        out_specs=vmem() + smem() + vmem(),
        scratch_shapes=[
            pltpu.SMEM((SLOTS, ROWS), jnp.int32),
            pltpu.SMEM((ROWS,), jnp.int32),
            pltpu.VMEM((ENTRIES, BLK, BLK), f32),
            pltpu.SemaphoreType.DMA((ROWS // 2,)),
            pltpu.SemaphoreType.DMA((2,)),
        ]
        + PARTIAL,
        compiler_params=params(),
        cost_estimate=cost(10**10),
        name="setup",
    )(columns, lengths, send, values, concentration, rate)
    turned = pltpu.with_memory_space_constraint(turned, pltpu.VMEM)
    table = pltpu.with_memory_space_constraint(table, pltpu.SMEM)
    basis = []

    for k in range(DEGREE):
        field, *packets = pl.pallas_call(
            far_part(k == 0),
            out_shape=[FIELD] + PACKETS,
            in_specs=smem() + vmem(6),
            out_specs=vmem(5),
            scratch_shapes=PARTIAL,
            compiler_params=params(),
            name="far_part",
        )(table, turned, near, *arrived)
        basis.append(field)
        arrived = exchange(packets, k + 1)
        near = pl.pallas_call(
            near_part,
            out_shape=FIELD,
            in_specs=smem() + vmem(4),
            out_specs=vmem()[0],
            scratch_shapes=PARTIAL,
            compiler_params=params(),
            cost_estimate=cost(10**10),
            name="near_part",
        )(table, turned, field, rate, concentration)
    sums = pl.pallas_call(
        last_part,
        out_shape=jax.ShapeDtypeStruct((devices, ROWS), f32),
        in_specs=smem() + vmem(6 + DEGREE),
        out_specs=vmem()[0],
        scratch_shapes=[pltpu.VMEM((ROWS, BLK), f32), pltpu.VMEM((ROWS, BLK), f32)] + PARTIAL,
        compiler_params=params(),
        name="last_part",
    )(table, turned, near, *arrived, *basis)
    everyone = lax.all_to_all(sums, "dom", split_axis=0, concat_axis=0, tiled=True)
    return pl.pallas_call(
        finish,
        out_shape=FIELD,
        in_specs=smem() + vmem(2 + DEGREE),
        out_specs=vmem()[0],
        compiler_params=params(),
        name="finish",
    )(step, everyone, concentration, *basis)


def solution(mesh):
    shifts, swaps = exchanges(mesh.shape["dom"])

    def run(*arrays):
        return shards(shifts, swaps, *arrays)

    split = P("dom")
    return jax.shard_map(
        run,
        mesh=mesh,
        in_specs=(split, split, P(), split, split, split, split),
        out_specs=split,
        check_vma=False,
    )
```

```python
import jax
import jax.numpy as jnp
from jax import lax
from jax.experimental import pallas as pl
from jax.experimental.pallas import tpu as pltpu
from jax.sharding import PartitionSpec as P

BLK = 128
ROWS = 32
SLOTS = 5
GHOST = 16
ENTRIES = ROWS * SLOTS
DEGREE = 6
SHIFT = 8.0
SCALE = 0.25
PAIRS = [(a, b) for b in range(DEGREE + 1) for a in range(min(b, DEGREE - 1) + 1)]

OFFSETS = (-2, -1, 1, 2)
FIRST_INDICES = (2, 3, 0, 1)
EIGHT = 8
EXCHANGES = (
    ((2, 1), (5, 6)),
    ((2, 0), (3, 1), (4, 6), (5, 7)),
    ((6, 8), (8, 6), (7, 9), (9, 7), (2, 4), (4, 2), (3, 5), (5, 3)),
    ((7, 8), (8, 7), (3, 4), (4, 3), (1, 2), (6, 5)),
    ((0, 1), (1, 0), (2, 3), (3, 2), (4, 5), (5, 4), (6, 7), (7, 6)),
    ((0, 2), (1, 3), (6, 4), (7, 5)),
)
TURNS = len(EXCHANGES)
FAR_BY = (2, 3)
MID_BY = (0, 1, 4, 5)

GROUPS = (80, 32, 40)
LIST = ENTRIES + max(GROUPS)
NEAR = 0
FAR = 3 * LIST
MID = 6 * LIST
REST = 9 * LIST
SEND = REST + 3 * LIST
COUNTS = SEND + TURNS * GHOST
BY = COUNTS + 4
TABLE = BY + 4
LINES = TURNS * GHOST


f32 = jnp.float32
bf16 = jnp.bfloat16


def vmem(n=1):
    return [pl.BlockSpec(memory_space=pltpu.VMEM)] * n


def smem(n=1):
    return [pl.BlockSpec(memory_space=pltpu.SMEM)] * n


def exchanges(devices):
    shifts = [[(p, (p + OFFSETS[q]) % devices) for p in range(devices)] for q in FIRST_INDICES]
    turns = [
        [((m + a) % devices, (m + b) % devices) for m in range(0, devices, EIGHT) for a, b in edges]
        for edges in EXCHANGES
    ]
    return shifts, turns


def looked_up(values):
    place = lax.axis_index("dom") % EIGHT
    found = jnp.int32(values[0])
    for i in range(1, EIGHT):
        found = jnp.where(place == i, jnp.int32(values[i]), found)
    return found


def arrivals():
    by = {
        (b % EIGHT, OFFSETS.index(b - a)): t for t, edges in enumerate(EXCHANGES) for a, b in edges
    }
    return [looked_up([by[r, q] for r in range(EIGHT)]) for q in range(4)]


def departures():
    by = {
        (a % EIGHT, t): OFFSETS.index(b - a) for t, edges in enumerate(EXCHANGES) for a, b in edges
    }
    return [looked_up([by.get((r, t), 0) for r in range(EIGHT)]) for t in range(TURNS)]


def write_packets(field, row_of, packets):
    for t in range(len(packets)):
        for g in range(GHOST):
            packets[t][g : g + 1, :] = field[pl.ds(row_of(t, g), 1), :]


def first_packets(send, concentration, rate, field, speed, table, p0, p1, p2, p3, done):
    copies = [
        pltpu.make_async_copy(send, table, done.at[0]),
        pltpu.make_async_copy(concentration, field, done.at[1]),
        pltpu.make_async_copy(rate, speed, done.at[2]),
    ]
    for copy in copies:
        copy.start()
    for copy in copies:
        copy.wait()
    write_packets(field, lambda t, g: table[0, FIRST_INDICES[t], g], (p0, p1, p2, p3))


def split(x):
    high = x.astype(bf16)
    return high, (x - high.astype(f32)).astype(bf16)


def setup(columns, lengths, send, values, field, rate, turned, table, out, where, length_of, blocks, done, small, *scratch):
    copies = [pltpu.make_async_copy(columns, where, small.at[0]), pltpu.make_async_copy(lengths, length_of, small.at[1])]
    for copy in copies:
        copy.start()

    def fetch(b):
        part = pl.ds(b * 2 * SLOTS, 2 * SLOTS)
        return pltpu.make_async_copy(values.at[part], blocks.at[part], done.at[b])

    for b in range(ROWS // 2):
        fetch(b).start()
    by = departures()
    at = arrivals()
    for q in range(4):
        table[BY + q] = at[q]
    for t in range(TURNS):
        for g in range(GHOST):
            table[SEND + t * GHOST + g] = send[0, by[t], g]
    for copy in copies:
        copy.wait()

    def rows(pair, carry):
        near, far, mid = carry
        fetch(pair).wait()
        for half in range(2):
            b = pair * 2 + half
            length = length_of[b]
            for s in range(SLOTS):
                column = where[s, b]
                index = jnp.maximum(column - ROWS, 0)
                q = index >> 4
                spot = jnp.where(q < 2, jnp.where(q == 0, at[0], at[1]), jnp.where(q == 2, at[2], at[3]))
                live = s < length
                ghost = jnp.logical_and(live, column >= ROWS)
                home = jnp.logical_and(live, column < ROWS)
                slow = jnp.logical_or(spot == FAR_BY[0], spot == FAR_BY[1])
                first = jnp.logical_and(ghost, slow)
                second = jnp.logical_and(ghost, jnp.logical_not(slow))
                base = jnp.where(
                    home, NEAR + near, jnp.where(first, FAR + far, jnp.where(second, MID + mid, REST))
                )
                table[base] = jnp.where(ghost, (spot << 4) + (index & 15), column)
                table[base + LIST] = b * SLOTS + s
                table[base + 2 * LIST] = b
                near = near + home.astype(jnp.int32)
                far = far + first.astype(jnp.int32)
                mid = mid + second.astype(jnp.int32)
        for s in range(2 * SLOTS):
            slot = pair * 2 * SLOTS + s
            high, rest = split(jnp.transpose(blocks[slot]))
            turned[slot, :, 0:BLK] = high
            turned[slot, :, BLK : 2 * BLK] = rest
        return near, far, mid

    zero = jnp.int32(0)
    counts = lax.fori_loop(0, ROWS // 2, rows, (zero, zero, zero))
    for i, base in enumerate((NEAR, FAR, MID)):
        table[COUNTS + i] = counts[i]
        for g in range(GROUPS[i]):
            table[base + counts[i] + g] = LINES
            table[base + LIST + counts[i] + g] = 0
            table[base + 2 * LIST + counts[i] + g] = 0
    fill((field,), (0,), *scratch)
    total = product(table, 0, turned, *scratch)
    out[...] = rate[...] * field[...] * (1.0 - field[...]) - total


def near_part(table, turned, field, rate, concentration, out, *scratch):
    fill((field,), (0,), *scratch)
    total = product(table, 0, turned, *scratch)
    slope = rate[...] * (1.0 - 2.0 * concentration[...]) + SHIFT
    out[...] = slope * field[...] - total


def fill(sources, turns, lines, *rest):
    for source, t in zip(sources, turns):
        start = pl.multiple_of(t * GHOST, GHOST)
        lines[pl.ds(start, source.shape[0]), :] = source[...]
    lines[LINES : LINES + 8, :] = jnp.zeros((8, BLK), f32)


def product(table, which, turned, lines, stage, *sums):
    base = (NEAR, FAR, MID)[which]
    size = GROUPS[which]
    count = table[COUNTS + which]
    for ref in sums:
        ref[...] = jnp.zeros((ROWS, BLK), f32)

    def group(c, carry):
        first = base + c * size
        for u in range(size):
            stage[u : u + 1, :] = lines[pl.ds(table[first + u], 1), :]
        for v in range(0, size, 8):
            left = jnp.concatenate(split(stage[v : v + 8, :]), axis=0)
            for u in range(v, v + 8):
                got = jnp.dot(left, turned[table[first + LIST + u]], preferred_element_type=f32)
                both = got[:, 0:BLK] + got[:, BLK : 2 * BLK]
                line = both[0:8] + both[8:16]
                to = pl.ds(table[first + 2 * LIST + u], 1)
                ref = sums[u % 4]
                ref[to, :] = ref[to, :] + line[u - v : u - v + 1, :]
        return carry

    lax.fori_loop(0, (count + size - 1) // size, group, 0)
    return (sums[0][...] + sums[1][...]) + (sums[2][...] + sums[3][...])


def middle_part(table, turned, near, g0, g1, g4, g5, out, *scratch):
    fill((g0, g1, g4, g5), MID_BY, *scratch)
    out[...] = near[...] - product(table, 2, turned, *scratch)


def send_out(table, out, packets):
    write_packets(out, lambda t, g: table[SEND + t * GHOST + g], packets)


def first_far_part(table, turned, near, g0, g1, g2, g3, out, *rest):
    packets, scratch = rest[:TURNS], rest[TURNS:]
    fill((g0, g1, g2, g3), [table[BY + q] for q in FIRST_INDICES], *scratch)
    out[...] = near[...] - product(table, 1, turned, *scratch)
    out[...] = out[...] - product(table, 2, turned, *scratch)
    send_out(table, out, packets)


def far_part(table, turned, near, g2, g3, out, *rest):
    packets, scratch = rest[:TURNS], rest[TURNS:]
    fill((g2, g3), FAR_BY, *scratch)
    out[...] = (near[...] - product(table, 1, turned, *scratch)) * SCALE
    send_out(table, out, packets)


def last_part(table, turned, near, g2, g3, *rest):
    basis = rest[:DEGREE]
    sums, out, rows, *scratch = rest[DEGREE:]
    fill((g2, g3), FAR_BY, *scratch)
    out[...] = (near[...] - product(table, 1, turned, *scratch)) * SCALE
    basis = basis + (out,)
    rows[...] = jnp.zeros(rows.shape, f32)
    for k, (a, b) in enumerate(PAIRS):
        both = basis[a][...] * basis[b][...]
        rows[k : k + 1, :] = jnp.sum(both, axis=0, keepdims=True)
    line = jnp.sum(jnp.transpose(rows[...]), axis=0, keepdims=True)
    sums[...] = jnp.broadcast_to(line, sums.shape)


def add(x, y):
    if x is None:
        return y
    return x if y is None else x + y


def times(x, y):
    return None if x is None or y is None else x * y


def minus(x, y):
    if y is None:
        return x
    return -y if x is None else x - y


def jacobian(v):
    out = [None if x is None else x * -SHIFT for x in v]
    for k in range(DEGREE):
        if v[k] is not None:
            out[k + 1] = add(out[k + 1], v[k] * (1.0 / SCALE))
    return out


def through(gram, v):
    return [
        (lambda terms: None if not terms else sum(terms[1:], terms[0]))(
            [gram[min(a, b), max(a, b)] * v[b] for b in range(DEGREE + 1) if v[b] is not None and (a, b) != (DEGREE, DEGREE)]
        )
        for a in range(DEGREE + 1)
    ]


def dot(u, v):
    terms = [x * y for x, y in zip(u, v) if x is not None and y is not None]
    return sum(terms[1:], terms[0])


def scaled(v, x):
    return [None if y is None else y * x for y in v]


def phi_weights(h, substep):
    n = len(h)
    reduced = [[None if x is None else x * substep * (1.0 / 64.0) for x in r] for r in h]
    matmul = lambda p, q: [
        [
            (lambda ts: None if not ts else sum(ts[1:], ts[0]))(
                [p[i][k] * q[k][j] for k in range(n) if p[i][k] is not None and q[k][j] is not None]
            )
            for j in range(n)
        ]
        for i in range(n)
    ]
    apply = lambda p, q: [
        (lambda ts: None if not ts else sum(ts[1:], ts[0]))(
            [p[i][k] * q[k] for k in range(n) if p[i][k] is not None and q[k] is not None]
        )
        for i in range(n)
    ]
    block = [[1.0 if i == j else None for j in range(n)] for i in range(n)]
    column = [None] * n
    for degree in range(12, 0, -1):
        inverse = 1.0 / degree
        block = matmul(reduced, block)
        block = [[None if x is None else x * inverse for x in r] for r in block]
        for i in range(n):
            block[i][i] = add(block[i][i], 1.0)
        column = apply(reduced, column)
        column[0] = add(column[0], 1.0 / 64.0)
        column = [None if x is None else x * inverse for x in column]
    for _ in range(6):
        moved = apply(block, column)
        column = [add(x, y) for x, y in zip(moved, column)]
        block = matmul(block, block)
    return column


def finish(step, everyone, concentration, *rest):
    basis, out = rest[:DEGREE], rest[DEGREE]
    total = jnp.sum(everyone[...], axis=0, keepdims=True)
    gram = {
        pair: jnp.broadcast_to(total[:, k : k + 1], (8, BLK)) for k, pair in enumerate(PAIRS)
    }
    substep = jnp.full((8, BLK), step[0] * 0.5, f32)
    one = jnp.ones((8, BLK), f32)
    forcing = [one] + [None] * DEGREE
    increment = [None] * (DEGREE + 1)
    for restart in range(2):
        start = forcing if restart == 0 else [add(x, y) for x, y in zip(jacobian(increment), forcing)]
        magnitude = jnp.sqrt(dot(start, through(gram, start)) + 1e-6)
        vectors = [scaled(start, 1.0 / magnitude)]
        hessenberg = [[None] * 3 for _ in range(3)]
        for j in range(3):
            mapped = jacobian(vectors[j])
            seen = through(gram, mapped)
            weights = [dot(v, seen) for v in vectors]
            for k, weight in enumerate(weights):
                hessenberg[k][j] = weight
            if j < 2:
                for v, weight in zip(vectors, weights):
                    mapped = [minus(x, times(y, weight)) for x, y in zip(mapped, v)]
                length = jnp.sqrt(dot(mapped, through(gram, mapped)) + 1e-6)
                hessenberg[j + 1][j] = length
                vectors.append(scaled(mapped, 1.0 / length))
        phi = phi_weights(hessenberg, substep)
        for v, weight in zip(vectors, phi):
            factor = substep * magnitude * weight
            increment = [add(x, times(y, factor)) for x, y in zip(increment, v)]
    for i in range(ROWS // 8):
        span = slice(8 * i, 8 * i + 8)
        line = concentration[span, :]
        for k in range(DEGREE):
            if increment[k] is not None:
                line = line + increment[k] * basis[k][span, :]
        out[span, :] = line


LIMIT = 24 << 20
FIELD = jax.ShapeDtypeStruct((ROWS, BLK), f32)
PACKET = jax.ShapeDtypeStruct((GHOST, BLK), f32)
PARTIAL = [
    pltpu.VMEM((LINES + 8, BLK), f32),
    pltpu.VMEM((max(GROUPS), BLK), f32),
] + [pltpu.VMEM((ROWS, BLK), f32)] * 4


def params():
    return pltpu.CompilerParams(vmem_limit_bytes=LIMIT)


def cost(flops):
    return pl.CostEstimate(flops=flops, bytes_accessed=0, transcendentals=0)


def hbm(n=1):
    return [pl.BlockSpec(memory_space=pltpu.HBM)] * n


def shards(shifts, turns, concentration, rate, step, values, columns, lengths, send):
    devices = BLK

    def exchange(packets, by):
        arrived = []
        for t in range(len(by)):
            arrived.append(lax.ppermute(packets[t], "dom", by[t]))
        return arrived

    def middle(near, arrived):
        return pl.pallas_call(
            middle_part,
            out_shape=FIELD,
            in_specs=smem() + vmem(6),
            out_specs=vmem()[0],
            scratch_shapes=PARTIAL,
            compiler_params=params(),
            cost_estimate=cost(10**9),
            name="middle_part",
        )(table, turned, near, *[arrived[t] for t in MID_BY])

    send, concentration, rate, values, columns, lengths = (
        pltpu.with_memory_space_constraint(x, pltpu.HBM)
        for x in (send, concentration, rate, values.reshape(ENTRIES, BLK, BLK), columns.T, lengths)
    )
    concentration, rate, send, *packets = pl.pallas_call(
        first_packets,
        out_shape=[FIELD, FIELD, pltpu.SMEM((1, 4, GHOST), jnp.int32)] + [PACKET] * 4,
        in_specs=hbm(3),
        out_specs=vmem(2) + smem() + vmem(4),
        scratch_shapes=[pltpu.SemaphoreType.DMA((3,))],
        compiler_params=params(),
        name="first_packets",
    )(send, concentration, rate)
    arrived = exchange(packets, shifts)
    send = pltpu.with_memory_space_constraint(send, pltpu.SMEM)
    turned, table, near = pl.pallas_call(
        setup,
        out_shape=[
            pltpu.VMEM((ENTRIES, BLK, 2 * BLK), bf16),
            pltpu.SMEM((TABLE,), jnp.int32),
            FIELD,
        ],
        in_specs=hbm(2) + smem() + hbm() + vmem(2),
        out_specs=vmem() + smem() + vmem(),
        scratch_shapes=[
            pltpu.SMEM((SLOTS, ROWS), jnp.int32),
            pltpu.SMEM((ROWS,), jnp.int32),
            pltpu.VMEM((ENTRIES, BLK, BLK), f32),
            pltpu.SemaphoreType.DMA((ROWS // 2,)),
            pltpu.SemaphoreType.DMA((2,)),
        ]
        + PARTIAL,
        compiler_params=params(),
        cost_estimate=cost(10**10),
        name="setup",
    )(columns, lengths, send, values, concentration, rate)
    turned = pltpu.with_memory_space_constraint(turned, pltpu.VMEM)
    table = pltpu.with_memory_space_constraint(table, pltpu.SMEM)
    basis = []

    for k in range(DEGREE):
        ghosts = arrived if k == 0 else [arrived[t] for t in FAR_BY]
        field, *packets = pl.pallas_call(
            far_part if k else first_far_part,
            out_shape=[FIELD] + [PACKET] * TURNS,
            in_specs=smem() + vmem(2 + len(ghosts)),
            out_specs=vmem(1 + TURNS),
            scratch_shapes=PARTIAL,
            compiler_params=params(),
            name="far_part",
        )(table, turned, near, *ghosts)
        basis.append(field)
        arrived = exchange(packets, turns)
        near = pl.pallas_call(
            near_part,
            out_shape=FIELD,
            in_specs=smem() + vmem(4),
            out_specs=vmem()[0],
            scratch_shapes=PARTIAL,
            compiler_params=params(),
            cost_estimate=cost(10**10),
            name="near_part",
        )(table, turned, field, rate, concentration)
        near = middle(near, arrived)
    sums = pl.pallas_call(
        last_part,
        out_shape=jax.ShapeDtypeStruct((devices, ROWS), f32),
        in_specs=smem() + vmem(4 + DEGREE),
        out_specs=vmem()[0],
        scratch_shapes=[pltpu.VMEM((ROWS, BLK), f32), pltpu.VMEM((ROWS, BLK), f32)] + PARTIAL,
        compiler_params=params(),
        name="last_part",
    )(table, turned, near, *[arrived[t] for t in FAR_BY], *basis)
    everyone = lax.all_to_all(sums, "dom", split_axis=0, concat_axis=0, tiled=True)
    return pl.pallas_call(
        finish,
        out_shape=FIELD,
        in_specs=smem() + vmem(2 + DEGREE),
        out_specs=vmem()[0],
        compiler_params=params(),
        name="finish",
    )(step, everyone, concentration, *basis)


def solution(mesh):
    shifts, turns = exchanges(mesh.shape["dom"])

    def run(*arrays):
        return shards(shifts, turns, *arrays)

    split = P("dom")
    return jax.shard_map(
        run,
        mesh=mesh,
        in_specs=(split, split, P(), split, split, split, split),
        out_specs=split,
        check_vma=False,
    )
```

```python
import jax
import jax.numpy as jnp
from jax import lax
from jax.experimental import pallas as pl
from jax.experimental.pallas import tpu as pltpu
from jax.sharding import PartitionSpec as P

BLK = 128
ROWS = 32
SLOTS = 5
GHOST = 16
ENTRIES = ROWS * SLOTS
DEGREE = 6
SHIFT = 8.0
SCALE = 0.25
PAIRS = [(a, b) for b in range(DEGREE + 1) for a in range(min(b, DEGREE - 1) + 1)]

OFFSETS = (-2, -1, 1, 2)
FIRST_INDICES = (2, 3, 0, 1)
EIGHT = 8
HOPS = (
    (1, -2, -2, -1, 2, -2, -2, -2),
    (-1, 2, -1, 1, -2, 1, -1, 1),
    (-2, 1, 2, 2, -1, 2, 2, 2),
    (2, -1, 1, -2, 1, -1, 1, -1),
)
EXCHANGES = tuple(tuple((r, r + hop) for r, hop in enumerate(hops)) for hops in HOPS)
TURNS = len(EXCHANGES)
FAR_BY = (2, 3)
MID_BY = (0, 1)

GROUPS = (80, 32, 32)
LIST = ENTRIES + max(GROUPS)
NEAR = 0
FAR = 3 * LIST
MID = 6 * LIST
REST = 9 * LIST
SEND = REST + 3 * LIST
COUNTS = SEND + TURNS * GHOST
BY = COUNTS + 4
TABLE = BY + 4
LINES = TURNS * GHOST

f32 = jnp.float32
bf16 = jnp.bfloat16


def vmem(n=1):
    return [pl.BlockSpec(memory_space=pltpu.VMEM)] * n


def smem(n=1):
    return [pl.BlockSpec(memory_space=pltpu.SMEM)] * n


def exchanges(devices):
    shifts = [[(p, (p + OFFSETS[q]) % devices) for p in range(devices)] for q in FIRST_INDICES]
    turns = [
        [((m + a) % devices, (m + b) % devices) for m in range(0, devices, EIGHT) for a, b in edges]
        for edges in EXCHANGES
    ]
    return shifts, turns


def looked_up(values):
    place = lax.axis_index("dom") % EIGHT
    found = jnp.int32(values[0])
    for i in range(1, EIGHT):
        found = jnp.where(place == i, jnp.int32(values[i]), found)
    return found


def arrivals():
    by = {
        (b % EIGHT, OFFSETS.index(b - a)): t for t, edges in enumerate(EXCHANGES) for a, b in edges
    }
    return [looked_up([by[r, q] for r in range(EIGHT)]) for q in range(4)]


def departures():
    by = {
        (a % EIGHT, t): OFFSETS.index(b - a) for t, edges in enumerate(EXCHANGES) for a, b in edges
    }
    return [looked_up([by.get((r, t), 0) for r in range(EIGHT)]) for t in range(TURNS)]


def write_packets(field, row_of, packets):
    for t in range(len(packets)):
        for g in range(GHOST):
            packets[t][g : g + 1, :] = field[pl.ds(row_of(t, g), 1), :]


def first_packets(send, concentration, rate, field, speed, table, p0, p1, p2, p3, done):
    copies = [
        pltpu.make_async_copy(send, table, done.at[0]),
        pltpu.make_async_copy(concentration, field, done.at[1]),
        pltpu.make_async_copy(rate, speed, done.at[2]),
    ]
    for copy in copies:
        copy.start()
    for copy in copies:
        copy.wait()
    write_packets(field, lambda t, g: table[0, FIRST_INDICES[t], g], (p0, p1, p2, p3))


def split(x):
    high = x.astype(bf16)
    return high, (x - high.astype(f32)).astype(bf16)


def setup(columns, lengths, send, values, field, rate, turned, table, out, where, length_of, blocks, done, small, *scratch):
    copies = [pltpu.make_async_copy(columns, where, small.at[0]), pltpu.make_async_copy(lengths, length_of, small.at[1])]
    for copy in copies:
        copy.start()

    def fetch(b):
        part = pl.ds(b * 2 * SLOTS, 2 * SLOTS)
        return pltpu.make_async_copy(values.at[part], blocks.at[part], done.at[b])

    for b in range(ROWS // 2):
        fetch(b).start()
    by = departures()
    at = arrivals()
    for q in range(4):
        table[BY + q] = at[q]
    for t in range(TURNS):
        for g in range(GHOST):
            table[SEND + t * GHOST + g] = send[0, by[t], g]
    for copy in copies:
        copy.wait()

    spots = (at[0] | (at[1] << 8)) | ((at[2] << 16) | (at[3] << 24))

    def listed(b, carry):
        near, far, mid = carry
        length = length_of[b]
        for s in range(SLOTS):
            column = where[s, b]
            index = jnp.maximum(column - ROWS, 0)
            spot = (spots >> ((index >> 4) << 3)) & 7
            live = s < length
            ghost = jnp.logical_and(live, column >= ROWS)
            home = jnp.logical_and(live, column < ROWS)
            first = jnp.logical_and(ghost, spot >= FAR_BY[0])
            second = jnp.logical_and(ghost, spot < FAR_BY[0])
            base = jnp.where(
                home, NEAR + near, jnp.where(first, FAR + far, jnp.where(second, MID + mid, REST))
            )
            table[base] = jnp.where(ghost, (spot << 4) + (index & 15), column)
            table[base + LIST] = b * SLOTS + s
            table[base + 2 * LIST] = b
            near = near + home.astype(jnp.int32)
            far = far + first.astype(jnp.int32)
            mid = mid + second.astype(jnp.int32)
        return near, far, mid

    def turn(pair, carry):
        fetch(pair).wait()
        for s in range(2 * SLOTS):
            slot = pair * 2 * SLOTS + s
            high, rest = split(jnp.transpose(blocks[slot]))
            turned[slot, :, 0:BLK] = high
            turned[slot, :, BLK : 2 * BLK] = rest
        return carry

    zero = jnp.int32(0)
    counts = lax.fori_loop(0, ROWS, listed, (zero, zero, zero))
    lax.fori_loop(0, ROWS // 2, turn, 0)
    for i, base in enumerate((NEAR, FAR, MID)):
        table[COUNTS + i] = counts[i]
        for g in range(GROUPS[i]):
            table[base + counts[i] + g] = LINES
            table[base + LIST + counts[i] + g] = 0
            table[base + 2 * LIST + counts[i] + g] = 0
    fill((field,), (0,), *scratch)
    total = product(table, 0, turned, *scratch)
    out[...] = rate[...] * field[...] * (1.0 - field[...]) - total


def near_part(table, turned, field, rate, concentration, out, *scratch):
    fill((field,), (0,), *scratch)
    total = product(table, 0, turned, *scratch)
    slope = rate[...] * (1.0 - 2.0 * concentration[...]) + SHIFT
    out[...] = slope * field[...] - total


def fill(sources, turns, lines, *rest):
    for source, t in zip(sources, turns):
        start = pl.multiple_of(t * GHOST, GHOST)
        lines[pl.ds(start, source.shape[0]), :] = source[...]
    lines[LINES : LINES + 8, :] = jnp.zeros((8, BLK), f32)


def product(table, which, turned, lines, stage, *sums):
    base = (NEAR, FAR, MID)[which]
    size = GROUPS[which]
    count = table[COUNTS + which]
    for ref in sums:
        ref[...] = jnp.zeros((ROWS, BLK), f32)

    def group(c, carry):
        first = base + c * size
        for u in range(size):
            stage[u : u + 1, :] = lines[pl.ds(table[first + u], 1), :]
        for v in range(0, size, 8):
            left = jnp.concatenate(split(stage[v : v + 8, :]), axis=0)
            for u in range(v, v + 8):
                got = jnp.dot(left, turned[table[first + LIST + u]], preferred_element_type=f32)
                both = got[:, 0:BLK] + got[:, BLK : 2 * BLK]
                line = both[0:8] + both[8:16]
                to = pl.ds(table[first + 2 * LIST + u], 1)
                ref = sums[u % 4]
                ref[to, :] = ref[to, :] + line[u - v : u - v + 1, :]
        return carry

    lax.fori_loop(0, (count + size - 1) // size, group, 0)
    return (sums[0][...] + sums[1][...]) + (sums[2][...] + sums[3][...])


def middle_part(table, turned, near, g0, g1, out, *scratch):
    fill((g0, g1), MID_BY, *scratch)
    out[...] = near[...] - product(table, 2, turned, *scratch)


def send_out(table, out, packets):
    write_packets(out, lambda t, g: table[SEND + t * GHOST + g], packets)


def first_far_part(table, turned, near, g0, g1, g2, g3, out, *rest):
    packets, scratch = rest[:TURNS], rest[TURNS:]
    fill((g0, g1, g2, g3), [table[BY + q] for q in FIRST_INDICES], *scratch)
    out[...] = near[...] - product(table, 1, turned, *scratch)
    out[...] = out[...] - product(table, 2, turned, *scratch)
    send_out(table, out, packets)


def far_part(table, turned, near, g2, g3, out, *rest):
    packets, scratch = rest[:TURNS], rest[TURNS:]
    fill((g2, g3), FAR_BY, *scratch)
    out[...] = (near[...] - product(table, 1, turned, *scratch)) * SCALE
    send_out(table, out, packets)


def inner_products(basis, pairs, rows, at):
    for k, (a, b) in enumerate(pairs):
        both = basis[a][...] * basis[b][...]
        rows[at + k : at + k + 1, :] = jnp.sum(both, axis=0, keepdims=True)


def gram_part(*refs):
    basis, rows = refs[:DEGREE], refs[DEGREE]
    rows[...] = jnp.zeros(rows.shape, f32)
    inner_products(basis, PAIRS[:-DEGREE], rows, 0)


def last_part(table, turned, near, g2, g3, *rest):
    basis = rest[:DEGREE]
    early, sums, out, rows, *scratch = rest[DEGREE:]
    fill((g2, g3), FAR_BY, *scratch)
    out[...] = (near[...] - product(table, 1, turned, *scratch)) * SCALE
    rows[...] = early[...]
    inner_products(basis + (out,), PAIRS[-DEGREE:], rows, len(PAIRS) - DEGREE)
    line = jnp.sum(jnp.transpose(rows[...]), axis=0, keepdims=True)
    sums[...] = jnp.broadcast_to(line, sums.shape)


def add(x, y):
    if x is None:
        return y
    return x if y is None else x + y


def times(x, y):
    return None if x is None or y is None else x * y


def minus(x, y):
    if y is None:
        return x
    return -y if x is None else x - y


def jacobian(v):
    out = [None if x is None else x * -SHIFT for x in v]
    for k in range(DEGREE):
        if v[k] is not None:
            out[k + 1] = add(out[k + 1], v[k] * (1.0 / SCALE))
    return out


def through(gram, v):
    return [
        (lambda terms: None if not terms else sum(terms[1:], terms[0]))(
            [gram[min(a, b), max(a, b)] * v[b] for b in range(DEGREE + 1) if v[b] is not None and (a, b) != (DEGREE, DEGREE)]
        )
        for a in range(DEGREE + 1)
    ]


def dot(u, v):
    terms = [x * y for x, y in zip(u, v) if x is not None and y is not None]
    return sum(terms[1:], terms[0])


def scaled(v, x):
    return [None if y is None else y * x for y in v]


def phi_weights(h, substep):
    n = len(h)
    reduced = [[None if x is None else x * substep * (1.0 / 64.0) for x in r] for r in h]
    matmul = lambda p, q: [
        [
            (lambda ts: None if not ts else sum(ts[1:], ts[0]))(
                [p[i][k] * q[k][j] for k in range(n) if p[i][k] is not None and q[k][j] is not None]
            )
            for j in range(n)
        ]
        for i in range(n)
    ]
    apply = lambda p, q: [
        (lambda ts: None if not ts else sum(ts[1:], ts[0]))(
            [p[i][k] * q[k] for k in range(n) if p[i][k] is not None and q[k] is not None]
        )
        for i in range(n)
    ]
    block = [[1.0 if i == j else None for j in range(n)] for i in range(n)]
    column = [None] * n
    for degree in range(12, 0, -1):
        inverse = 1.0 / degree
        block = matmul(reduced, block)
        block = [[None if x is None else x * inverse for x in r] for r in block]
        for i in range(n):
            block[i][i] = add(block[i][i], 1.0)
        column = apply(reduced, column)
        column[0] = add(column[0], 1.0 / 64.0)
        column = [None if x is None else x * inverse for x in column]
    for _ in range(6):
        moved = apply(block, column)
        column = [add(x, y) for x, y in zip(moved, column)]
        block = matmul(block, block)
    return column


def finish(step, everyone, concentration, *rest):
    basis, out = rest[:DEGREE], rest[DEGREE]
    total = jnp.sum(everyone[...], axis=0, keepdims=True)
    gram = {
        pair: jnp.broadcast_to(total[:, k : k + 1], (8, BLK)) for k, pair in enumerate(PAIRS)
    }
    substep = jnp.full((8, BLK), step[0] * 0.5, f32)
    one = jnp.ones((8, BLK), f32)
    forcing = [one] + [None] * DEGREE
    increment = [None] * (DEGREE + 1)
    for restart in range(2):
        start = forcing if restart == 0 else [add(x, y) for x, y in zip(jacobian(increment), forcing)]
        magnitude = jnp.sqrt(dot(start, through(gram, start)) + 1e-6)
        vectors = [scaled(start, 1.0 / magnitude)]
        hessenberg = [[None] * 3 for _ in range(3)]
        for j in range(3):
            mapped = jacobian(vectors[j])
            seen = through(gram, mapped)
            weights = [dot(v, seen) for v in vectors]
            for k, weight in enumerate(weights):
                hessenberg[k][j] = weight
            if j < 2:
                for v, weight in zip(vectors, weights):
                    mapped = [minus(x, times(y, weight)) for x, y in zip(mapped, v)]
                length = jnp.sqrt(dot(mapped, through(gram, mapped)) + 1e-6)
                hessenberg[j + 1][j] = length
                vectors.append(scaled(mapped, 1.0 / length))
        phi = phi_weights(hessenberg, substep)
        for v, weight in zip(vectors, phi):
            factor = substep * magnitude * weight
            increment = [add(x, times(y, factor)) for x, y in zip(increment, v)]
    for i in range(ROWS // 8):
        span = slice(8 * i, 8 * i + 8)
        line = concentration[span, :]
        for k in range(DEGREE):
            if increment[k] is not None:
                line = line + increment[k] * basis[k][span, :]
        out[span, :] = line


LIMIT = 24 << 20
FIELD = jax.ShapeDtypeStruct((ROWS, BLK), f32)
PACKET = jax.ShapeDtypeStruct((GHOST, BLK), f32)
PARTIAL = [
    pltpu.VMEM((LINES + 8, BLK), f32),
    pltpu.VMEM((max(GROUPS), BLK), f32),
] + [pltpu.VMEM((ROWS, BLK), f32)] * 4


def params():
    return pltpu.CompilerParams(vmem_limit_bytes=LIMIT)


def cost(flops):
    return pl.CostEstimate(flops=flops, bytes_accessed=0, transcendentals=0)


def hbm(n=1):
    return [pl.BlockSpec(memory_space=pltpu.HBM)] * n


def shards(shifts, turns, concentration, rate, step, values, columns, lengths, send):
    devices = BLK

    def exchange(packets, by):
        arrived = []
        for t in range(len(by)):
            arrived.append(lax.ppermute(packets[t], "dom", by[t]))
        return arrived

    def middle(near, arrived):
        return pl.pallas_call(
            middle_part,
            out_shape=FIELD,
            in_specs=smem() + vmem(2 + len(MID_BY)),
            out_specs=vmem()[0],
            scratch_shapes=PARTIAL,
            compiler_params=params(),
            cost_estimate=cost(10**9),
            name="middle_part",
        )(table, turned, near, *[arrived[t] for t in MID_BY])

    send, concentration, rate, values, columns, lengths = (
        pltpu.with_memory_space_constraint(x, pltpu.HBM)
        for x in (send, concentration, rate, values.reshape(ENTRIES, BLK, BLK), columns.T, lengths)
    )
    concentration, rate, send, *packets = pl.pallas_call(
        first_packets,
        out_shape=[FIELD, FIELD, pltpu.SMEM((1, 4, GHOST), jnp.int32)] + [PACKET] * 4,
        in_specs=hbm(3),
        out_specs=vmem(2) + smem() + vmem(4),
        scratch_shapes=[pltpu.SemaphoreType.DMA((3,))],
        compiler_params=params(),
        name="first_packets",
    )(send, concentration, rate)
    arrived = exchange(packets, shifts)
    send = pltpu.with_memory_space_constraint(send, pltpu.SMEM)
    turned, table, near = pl.pallas_call(
        setup,
        out_shape=[
            pltpu.VMEM((ENTRIES, BLK, 2 * BLK), bf16),
            pltpu.SMEM((TABLE,), jnp.int32),
            FIELD,
        ],
        in_specs=hbm(2) + smem() + hbm() + vmem(2),
        out_specs=vmem() + smem() + vmem(),
        scratch_shapes=[
            pltpu.SMEM((SLOTS, ROWS), jnp.int32),
            pltpu.SMEM((ROWS,), jnp.int32),
            pltpu.VMEM((ENTRIES, BLK, BLK), f32),
            pltpu.SemaphoreType.DMA((ROWS // 2,)),
            pltpu.SemaphoreType.DMA((2,)),
        ]
        + PARTIAL,
        compiler_params=params(),
        cost_estimate=cost(10**10),
        name="setup",
    )(columns, lengths, send, values, concentration, rate)
    turned = pltpu.with_memory_space_constraint(turned, pltpu.VMEM)
    table = pltpu.with_memory_space_constraint(table, pltpu.SMEM)
    basis = []

    for k in range(DEGREE):
        ghosts = arrived if k == 0 else [arrived[t] for t in FAR_BY]
        field, *packets = pl.pallas_call(
            far_part if k else first_far_part,
            out_shape=[FIELD] + [PACKET] * TURNS,
            in_specs=smem() + vmem(2 + len(ghosts)),
            out_specs=vmem(1 + TURNS),
            scratch_shapes=PARTIAL,
            compiler_params=params(),
            name="far_part",
        )(table, turned, near, *ghosts)
        basis.append(field)
        arrived = exchange(packets, turns)
        near = pl.pallas_call(
            near_part,
            out_shape=FIELD,
            in_specs=smem() + vmem(4),
            out_specs=vmem()[0],
            scratch_shapes=PARTIAL,
            compiler_params=params(),
            cost_estimate=cost(10**10),
            name="near_part",
        )(table, turned, field, rate, concentration)
        near = middle(near, arrived)
    early = pl.pallas_call(
        gram_part,
        out_shape=FIELD,
        in_specs=vmem(DEGREE),
        out_specs=vmem()[0],
        compiler_params=params(),
        cost_estimate=cost(10**9),
        name="gram_part",
    )(*basis)
    sums = pl.pallas_call(
        last_part,
        out_shape=jax.ShapeDtypeStruct((devices, ROWS), f32),
        in_specs=smem() + vmem(5 + DEGREE),
        out_specs=vmem()[0],
        scratch_shapes=[pltpu.VMEM((ROWS, BLK), f32), pltpu.VMEM((ROWS, BLK), f32)] + PARTIAL,
        compiler_params=params(),
        name="last_part",
    )(table, turned, near, *[arrived[t] for t in FAR_BY], *basis, early)
    everyone = lax.all_to_all(sums, "dom", split_axis=0, concat_axis=0, tiled=True)
    return pl.pallas_call(
        finish,
        out_shape=FIELD,
        in_specs=smem() + vmem(2 + DEGREE),
        out_specs=vmem()[0],
        compiler_params=params(),
        name="finish",
    )(step, everyone, concentration, *basis)


def solution(mesh):
    shifts, turns = exchanges(mesh.shape["dom"])

    def run(*arrays):
        return shards(shifts, turns, *arrays)

    split = P("dom")
    return jax.shard_map(
        run,
        mesh=mesh,
        in_specs=(split, split, P(), split, split, split, split),
        out_specs=split,
        check_vma=False,
    )
```

```python
import math

import jax
import jax.numpy as jnp
from jax import lax
from jax.experimental import pallas as pl
from jax.experimental.pallas import tpu as pltpu
from jax.sharding import PartitionSpec as P

BLK = 128
ROWS = 32
SLOTS = 5
GHOST = 16
ENTRIES = ROWS * SLOTS
DEGREE = 6
SHIFT = 8.0
SCALE = 0.25
PAIRS = [(a, b) for b in range(DEGREE + 1) for a in range(min(b, DEGREE - 1) + 1)]

OFFSETS = (-2, -1, 1, 2)
FIRST_INDICES = (2, 3, 0, 1)
EIGHT = 8
HOPS = (
    (1, -2, -2, -1, 2, -2, -2, -2),
    (-1, 2, -1, 1, -2, 1, -1, 1),
    (-2, 1, 2, 2, -1, 2, 2, 2),
    (2, -1, 1, -2, 1, -1, 1, -1),
)
EXCHANGES = tuple(tuple((r, r + hop) for r, hop in enumerate(hops)) for hops in HOPS)
TURNS = len(EXCHANGES)
FAR_BY = (2, 3)
MID_BY = (0, 1)

GROUPS = (80, 32, 32)
LIST = ENTRIES + max(GROUPS)
NEAR = 0
FAR = 3 * LIST
MID = 6 * LIST
REST = 9 * LIST
SEND = REST + 3 * LIST
COUNTS = SEND + TURNS * GHOST
BY = COUNTS + 4
TABLE = BY + 4
LINES = TURNS * GHOST

f32 = jnp.float32
bf16 = jnp.bfloat16


def vmem(n=1):
    return [pl.BlockSpec(memory_space=pltpu.VMEM)] * n


def smem(n=1):
    return [pl.BlockSpec(memory_space=pltpu.SMEM)] * n


def exchanges(devices):
    shifts = [[(p, (p + OFFSETS[q]) % devices) for p in range(devices)] for q in FIRST_INDICES]
    turns = [
        [((m + a) % devices, (m + b) % devices) for m in range(0, devices, EIGHT) for a, b in edges]
        for edges in EXCHANGES
    ]
    return shifts, turns


def looked_up(values):
    place = lax.axis_index("dom") % EIGHT
    found = jnp.int32(values[0])
    for i in range(1, EIGHT):
        found = jnp.where(place == i, jnp.int32(values[i]), found)
    return found


def arrivals():
    by = {
        (b % EIGHT, OFFSETS.index(b - a)): t for t, edges in enumerate(EXCHANGES) for a, b in edges
    }
    return [looked_up([by[r, q] for r in range(EIGHT)]) for q in range(4)]


def departures():
    by = {
        (a % EIGHT, t): OFFSETS.index(b - a) for t, edges in enumerate(EXCHANGES) for a, b in edges
    }
    return [looked_up([by.get((r, t), 0) for r in range(EIGHT)]) for t in range(TURNS)]


def write_packets(field, row_of, packets):
    for t in range(len(packets)):
        for g in range(GHOST):
            packets[t][g : g + 1, :] = field[pl.ds(row_of(t, g), 1), :]


def first_packets(send, concentration, rate, field, speed, table, p0, p1, p2, p3, done):
    copies = [
        pltpu.make_async_copy(send, table, done.at[0]),
        pltpu.make_async_copy(concentration, field, done.at[1]),
        pltpu.make_async_copy(rate, speed, done.at[2]),
    ]
    for copy in copies:
        copy.start()
    for copy in copies:
        copy.wait()
    write_packets(field, lambda t, g: table[0, FIRST_INDICES[t], g], (p0, p1, p2, p3))


def split(x):
    high = x.astype(bf16)
    return high, (x - high.astype(f32)).astype(bf16)


def setup(columns, lengths, send, values, field, rate, turned, table, out, where, length_of, blocks, done, small, *scratch):
    copies = [pltpu.make_async_copy(columns, where, small.at[0]), pltpu.make_async_copy(lengths, length_of, small.at[1])]
    for copy in copies:
        copy.start()

    def fetch(b):
        part = pl.ds(b * 2 * SLOTS, 2 * SLOTS)
        return pltpu.make_async_copy(values.at[part], blocks.at[part], done.at[b])

    for b in range(ROWS // 2):
        fetch(b).start()
    by = departures()
    at = arrivals()
    for q in range(4):
        table[BY + q] = at[q]
    for t in range(TURNS):
        for g in range(GHOST):
            table[SEND + t * GHOST + g] = send[0, by[t], g]
    for copy in copies:
        copy.wait()

    spots = (at[0] | (at[1] << 8)) | ((at[2] << 16) | (at[3] << 24))

    def rows(pair, carry):
        near, far, mid = carry
        fetch(pair).wait()
        for half in range(2):
            b = pair * 2 + half
            length = length_of[b]
            for s in range(SLOTS):
                column = where[s, b]
                index = jnp.maximum(column - ROWS, 0)
                spot = (spots >> ((index >> 4) << 3)) & 7
                live = s < length
                ghost = jnp.logical_and(live, column >= ROWS)
                home = jnp.logical_and(live, column < ROWS)
                first = jnp.logical_and(ghost, spot >= FAR_BY[0])
                second = jnp.logical_and(ghost, spot < FAR_BY[0])
                base = jnp.where(
                    home, NEAR + near, jnp.where(first, FAR + far, jnp.where(second, MID + mid, REST))
                )
                table[base] = jnp.where(ghost, (spot << 4) + (index & 15), column)
                table[base + LIST] = b * SLOTS + s
                table[base + 2 * LIST] = b
                near = near + home.astype(jnp.int32)
                far = far + first.astype(jnp.int32)
                mid = mid + second.astype(jnp.int32)
        for s in range(2 * SLOTS):
            slot = pair * 2 * SLOTS + s
            high, rest = split(jnp.transpose(blocks[slot]))
            turned[slot, :, 0:BLK] = high
            turned[slot, :, BLK : 2 * BLK] = rest
        return near, far, mid

    zero = jnp.int32(0)
    counts = lax.fori_loop(0, ROWS // 2, rows, (zero, zero, zero))
    for i, base in enumerate((NEAR, FAR, MID)):
        table[COUNTS + i] = counts[i]
        for g in range(GROUPS[i]):
            table[base + counts[i] + g] = LINES
            table[base + LIST + counts[i] + g] = 0
            table[base + 2 * LIST + counts[i] + g] = 0
    fill((field,), (0,), *scratch)
    total = product(table, 0, turned, *scratch)
    out[...] = rate[...] * field[...] * (1.0 - field[...]) - total


def near_part(table, turned, field, rate, concentration, out, *scratch):
    fill((field,), (0,), *scratch)
    total = product(table, 0, turned, *scratch)
    slope = rate[...] * (1.0 - 2.0 * concentration[...]) + SHIFT
    out[...] = slope * field[...] - total


def fill(sources, turns, lines, *rest):
    for source, t in zip(sources, turns):
        start = pl.multiple_of(t * GHOST, GHOST)
        lines[pl.ds(start, source.shape[0]), :] = source[...]
    lines[LINES : LINES + 8, :] = jnp.zeros((8, BLK), f32)


def product(table, which, turned, lines, stage, *sums):
    base = (NEAR, FAR, MID)[which]
    size = GROUPS[which]
    count = table[COUNTS + which]
    for ref in sums:
        ref[...] = jnp.zeros((ROWS, BLK), f32)

    def group(c, carry):
        first = base + c * size
        for u in range(size):
            stage[u : u + 1, :] = lines[pl.ds(table[first + u], 1), :]
        for v in range(0, size, 8):
            left = jnp.concatenate(split(stage[v : v + 8, :]), axis=0)
            for u in range(v, v + 8):
                got = jnp.dot(left, turned[table[first + LIST + u]], preferred_element_type=f32)
                both = got[:, 0:BLK] + got[:, BLK : 2 * BLK]
                line = both[0:8] + both[8:16]
                to = pl.ds(table[first + 2 * LIST + u], 1)
                ref = sums[u % 4]
                ref[to, :] = ref[to, :] + line[u - v : u - v + 1, :]
        return carry

    lax.fori_loop(0, (count + size - 1) // size, group, 0)
    return (sums[0][...] + sums[1][...]) + (sums[2][...] + sums[3][...])


def middle_part(table, turned, near, g0, g1, out, *scratch):
    fill((g0, g1), MID_BY, *scratch)
    out[...] = near[...] - product(table, 2, turned, *scratch)


def send_out(table, out, packets):
    write_packets(out, lambda t, g: table[SEND + t * GHOST + g], packets)


def first_far_part(table, turned, near, g0, g1, g2, g3, out, *rest):
    packets, scratch = rest[:TURNS], rest[TURNS:]
    fill((g0, g1, g2, g3), [table[BY + q] for q in FIRST_INDICES], *scratch)
    out[...] = near[...] - product(table, 1, turned, *scratch)
    out[...] = out[...] - product(table, 2, turned, *scratch)
    send_out(table, out, packets)


def far_part(table, turned, near, g2, g3, out, *rest):
    packets, scratch = rest[:TURNS], rest[TURNS:]
    fill((g2, g3), FAR_BY, *scratch)
    out[...] = (near[...] - product(table, 1, turned, *scratch)) * SCALE
    send_out(table, out, packets)


def inner_products(basis, pairs, rows, at):
    for k, (a, b) in enumerate(pairs):
        both = basis[a][...] * basis[b][...]
        rows[at + k : at + k + 1, :] = jnp.sum(both, axis=0, keepdims=True)


def gram_part(*refs):
    basis, rows = refs[:DEGREE], refs[DEGREE]
    rows[...] = jnp.zeros(rows.shape, f32)
    inner_products(basis, PAIRS[:-DEGREE], rows, 0)


def last_part(table, turned, near, g2, g3, *rest):
    basis = rest[:DEGREE]
    early, sums, out, rows, *scratch = rest[DEGREE:]
    fill((g2, g3), FAR_BY, *scratch)
    out[...] = (near[...] - product(table, 1, turned, *scratch)) * SCALE
    rows[...] = early[...]
    inner_products(basis + (out,), PAIRS[-DEGREE:], rows, len(PAIRS) - DEGREE)
    line = jnp.sum(jnp.transpose(rows[...]), axis=0, keepdims=True)
    sums[...] = jnp.broadcast_to(line, sums.shape)


def add(x, y):
    if x is None:
        return y
    return x if y is None else x + y


def times(x, y):
    return None if x is None or y is None else x * y


def minus(x, y):
    if y is None:
        return x
    return -y if x is None else x - y


def jacobian(v):
    out = [None if x is None else x * -SHIFT for x in v]
    for k in range(DEGREE):
        if v[k] is not None:
            out[k + 1] = add(out[k + 1], v[k] * (1.0 / SCALE))
    return out


def tree(terms):
    terms = list(terms)
    while len(terms) > 1:
        odd = [terms[-1]] if len(terms) % 2 else []
        terms = [x + y for x, y in zip(terms[::2], terms[1::2])] + odd
    return terms[0] if terms else None


def through(gram, v):
    return [
        tree(
            [gram[min(a, b), max(a, b)] * v[b] for b in range(DEGREE + 1) if v[b] is not None and (a, b) != (DEGREE, DEGREE)]
        )
        for a in range(DEGREE + 1)
    ]


def dot(u, v):
    return tree([x * y for x, y in zip(u, v) if x is not None and y is not None])


def scaled(v, x):
    return [None if y is None else y * x for y in v]


def phi_weights(h, substep):
    n = len(h)
    one = [[None if x is None else x * substep * (1.0 / 64.0) for x in r] for r in h]

    def matmul(p, q):
        pick = lambda i, j: [p[i][k] * q[k][j] for k in range(n) if p[i][k] is not None]
        return [[tree(pick(i, j)) for j in range(n)] for i in range(n)]

    def apply(p, q):
        return [tree([p[i][k] * q[k] for k in range(n)]) for i in range(n)]

    two = [
        [tree([one[i][k] * one[k][j] for k in range(n) if one[i][k] is not None and one[k][j] is not None]) for j in range(n)]
        for i in range(n)
    ]
    three = matmul(one, two)
    factor = [1.0 / math.factorial(k) for k in range(13)]

    def low(i, j, k):
        total = add(None if one[i][j] is None else one[i][j] * factor[k + 1], two[i][j] * factor[k + 2])
        return total + factor[k] if i == j else total

    def low_column(i, k):
        total = add(None if one[i][0] is None else one[i][0] * factor[k + 1], two[i][0] * factor[k + 2])
        return total + factor[k] if i == 0 else total

    block = [[three[i][j] * factor[12] + low(i, j, 9) for j in range(n)] for i in range(n)]
    column = [low_column(i, 10) for i in range(n)]
    for k in (6, 3, 0):
        block, column = matmul(three, block), apply(three, column)
        block = [[block[i][j] + low(i, j, k) for j in range(n)] for i in range(n)]
        column = [column[i] + low_column(i, k + 1) for i in range(n)]
    column = [x * (1.0 / 64.0) for x in column]
    for turn in range(6):
        moved = apply(block, column)
        column = [x + y for x, y in zip(moved, column)]
        if turn < 5:
            block = matmul(block, block)
    return column


def finish(step, everyone, concentration, *rest):
    basis, out = rest[:DEGREE], rest[DEGREE]
    total = jnp.sum(everyone[...], axis=0, keepdims=True)
    gram = {
        pair: jnp.broadcast_to(total[:, k : k + 1], (8, BLK)) for k, pair in enumerate(PAIRS)
    }
    substep = jnp.full((8, BLK), step[0] * 0.5, f32)
    one = jnp.ones((8, BLK), f32)
    forcing = [one] + [None] * DEGREE
    increment = [None] * (DEGREE + 1)
    for restart in range(2):
        start = forcing if restart == 0 else [add(x, y) for x, y in zip(jacobian(increment), forcing)]
        magnitude = jnp.sqrt(dot(start, through(gram, start)) + 1e-6)
        vectors = [scaled(start, 1.0 / magnitude)]
        hessenberg = [[None] * 3 for _ in range(3)]
        for j in range(3):
            mapped = jacobian(vectors[j])
            seen = through(gram, mapped)
            weights = [dot(v, seen) for v in vectors]
            for k, weight in enumerate(weights):
                hessenberg[k][j] = weight
            if j < 2:
                for v, weight in zip(vectors, weights):
                    mapped = [minus(x, times(y, weight)) for x, y in zip(mapped, v)]
                length = jnp.sqrt(dot(mapped, through(gram, mapped)) + 1e-6)
                hessenberg[j + 1][j] = length
                vectors.append(scaled(mapped, 1.0 / length))
        phi = phi_weights(hessenberg, substep)
        for v, weight in zip(vectors, phi):
            factor = substep * magnitude * weight
            increment = [add(x, times(y, factor)) for x, y in zip(increment, v)]
    for i in range(ROWS // 8):
        span = slice(8 * i, 8 * i + 8)
        line = concentration[span, :]
        for k in range(DEGREE):
            if increment[k] is not None:
                line = line + increment[k] * basis[k][span, :]
        out[span, :] = line


LIMIT = 24 << 20
FIELD = jax.ShapeDtypeStruct((ROWS, BLK), f32)
PACKET = jax.ShapeDtypeStruct((GHOST, BLK), f32)
PARTIAL = [
    pltpu.VMEM((LINES + 8, BLK), f32),
    pltpu.VMEM((max(GROUPS), BLK), f32),
] + [pltpu.VMEM((ROWS, BLK), f32)] * 4


def params():
    return pltpu.CompilerParams(vmem_limit_bytes=LIMIT)


def cost(flops):
    return pl.CostEstimate(flops=flops, bytes_accessed=0, transcendentals=0)


def hbm(n=1):
    return [pl.BlockSpec(memory_space=pltpu.HBM)] * n


def shards(shifts, turns, concentration, rate, step, values, columns, lengths, send):
    devices = BLK

    def exchange(packets, by):
        arrived = []
        for t in range(len(by)):
            arrived.append(lax.ppermute(packets[t], "dom", by[t]))
        return arrived

    def middle(near, arrived):
        return pl.pallas_call(
            middle_part,
            out_shape=FIELD,
            in_specs=smem() + vmem(2 + len(MID_BY)),
            out_specs=vmem()[0],
            scratch_shapes=PARTIAL,
            compiler_params=params(),
            cost_estimate=cost(10**9),
            name="middle_part",
        )(table, turned, near, *[arrived[t] for t in MID_BY])

    send, concentration, rate, values, columns, lengths = (
        pltpu.with_memory_space_constraint(x, pltpu.HBM)
        for x in (send, concentration, rate, values.reshape(ENTRIES, BLK, BLK), columns.T, lengths)
    )
    concentration, rate, send, *packets = pl.pallas_call(
        first_packets,
        out_shape=[FIELD, FIELD, pltpu.SMEM((1, 4, GHOST), jnp.int32)] + [PACKET] * 4,
        in_specs=hbm(3),
        out_specs=vmem(2) + smem() + vmem(4),
        scratch_shapes=[pltpu.SemaphoreType.DMA((3,))],
        compiler_params=params(),
        name="first_packets",
    )(send, concentration, rate)
    arrived = exchange(packets, shifts)
    send = pltpu.with_memory_space_constraint(send, pltpu.SMEM)
    turned, table, near = pl.pallas_call(
        setup,
        out_shape=[
            pltpu.VMEM((ENTRIES, BLK, 2 * BLK), bf16),
            pltpu.SMEM((TABLE,), jnp.int32),
            FIELD,
        ],
        in_specs=hbm(2) + smem() + hbm() + vmem(2),
        out_specs=vmem() + smem() + vmem(),
        scratch_shapes=[
            pltpu.SMEM((SLOTS, ROWS), jnp.int32),
            pltpu.SMEM((ROWS,), jnp.int32),
            pltpu.VMEM((ENTRIES, BLK, BLK), f32),
            pltpu.SemaphoreType.DMA((ROWS // 2,)),
            pltpu.SemaphoreType.DMA((2,)),
        ]
        + PARTIAL,
        compiler_params=params(),
        cost_estimate=cost(10**10),
        name="setup",
    )(columns, lengths, send, values, concentration, rate)
    turned = pltpu.with_memory_space_constraint(turned, pltpu.VMEM)
    table = pltpu.with_memory_space_constraint(table, pltpu.SMEM)
    basis = []

    for k in range(DEGREE):
        ghosts = arrived if k == 0 else [arrived[t] for t in FAR_BY]
        field, *packets = pl.pallas_call(
            far_part if k else first_far_part,
            out_shape=[FIELD] + [PACKET] * TURNS,
            in_specs=smem() + vmem(2 + len(ghosts)),
            out_specs=vmem(1 + TURNS),
            scratch_shapes=PARTIAL,
            compiler_params=params(),
            name="far_part",
        )(table, turned, near, *ghosts)
        basis.append(field)
        arrived = exchange(packets, turns)
        near = pl.pallas_call(
            near_part,
            out_shape=FIELD,
            in_specs=smem() + vmem(4),
            out_specs=vmem()[0],
            scratch_shapes=PARTIAL,
            compiler_params=params(),
            cost_estimate=cost(10**10),
            name="near_part",
        )(table, turned, field, rate, concentration)
        near = middle(near, arrived)
    early = pl.pallas_call(
        gram_part,
        out_shape=FIELD,
        in_specs=vmem(DEGREE),
        out_specs=vmem()[0],
        compiler_params=params(),
        cost_estimate=cost(10**9),
        name="gram_part",
    )(*basis)
    sums = pl.pallas_call(
        last_part,
        out_shape=jax.ShapeDtypeStruct((devices, ROWS), f32),
        in_specs=smem() + vmem(5 + DEGREE),
        out_specs=vmem()[0],
        scratch_shapes=[pltpu.VMEM((ROWS, BLK), f32), pltpu.VMEM((ROWS, BLK), f32)] + PARTIAL,
        compiler_params=params(),
        name="last_part",
    )(table, turned, near, *[arrived[t] for t in FAR_BY], *basis, early)
    everyone = lax.all_to_all(sums, "dom", split_axis=0, concat_axis=0, tiled=True)
    return pl.pallas_call(
        finish,
        out_shape=FIELD,
        in_specs=smem() + vmem(2 + DEGREE),
        out_specs=vmem()[0],
        compiler_params=params(),
        name="finish",
    )(step, everyone, concentration, *basis)


def solution(mesh):
    shifts, turns = exchanges(mesh.shape["dom"])

    def run(*arrays):
        return shards(shifts, turns, *arrays)

    split = P("dom")
    return jax.shard_map(
        run,
        mesh=mesh,
        in_specs=(split, split, P(), split, split, split, split),
        out_specs=split,
        check_vma=False,
    )
```
